32 devices in a mesh: dp: 8 (over z, y), inner: 4 (over x, core).
Axes of the slice: x: 2, y: 2, z: 4, core: 2. Of those that a mesh axis runs over, the one named last changes fastest.
Arguments:
- tokens: bfloat16 [32, 320, 1152], P(('dp', 'inner')), may hold values from -6 to 6
- time_vec: bfloat16 [32, 1152], P(('dp', 'inner')), may hold values from -6 to 6
- grid: int32 [32, 2], P(('dp', 'inner')), may hold values from 6 to 32, as said below
- cotangent: bfloat16 [32, 320, 1152], P(('dp', 'inner')), may hold values from -6 to 6
- gain_attn: float32 [1152], replicated, may hold values from 0.1 to 1.9
- gain_mlp: float32 [1152], replicated, may hold values from 0.1 to 1.9
- w_query: bfloat16 [1152, 1152], P('inner', 'dp'), may hold values from -0.1875 to 0.1875
- w_key: bfloat16 [1152, 1152], P('inner', 'dp'), may hold values from -0.1875 to 0.1875
- w_value: bfloat16 [1152, 1152], P('inner', 'dp'), may hold values from -0.1875 to 0.1875
- w_time_query: bfloat16 [1152, 1152], P('inner', 'dp'), may hold values from -0.1875 to 0.1875
- w_time_value: bfloat16 [1152, 1152], P('inner', 'dp'), may hold values from -0.1875 to 0.1875
- w_out: bfloat16 [1152, 1152], P('inner', 'dp'), may hold values from -1 to 1
- w_up: bfloat16 [1152, 4608], P('inner', 'dp'), may hold values from -0.1875 to 0.1875
- w_down: bfloat16 [4608, 1152], P('inner', 'dp'), may hold values from -0.09375 to 0.09375
- bias_rows: float32 [16, 63], replicated, may hold values from -3 to 3
- bias_cols: float32 [16, 63], replicated, may hold values from -3 to 3
Outputs:
- output: bfloat16 [32, 320, 1152], P(('dp', 'inner'))
- grad_tokens: bfloat16 [32, 320, 1152], P(('dp', 'inner'))
- grad_gain_attn: float32 [1152], replicated
- grad_gain_mlp: float32 [1152], replicated
- grad_w_query: float32 [1152, 1152], P('inner', 'dp')
- grad_w_key: float32 [1152, 1152], P('inner', 'dp')
- grad_w_value: float32 [1152, 1152], P('inner', 'dp')
- grad_w_time_query: float32 [1152, 1152], P('inner', 'dp')
- grad_w_time_value: float32 [1152, 1152], P('inner', 'dp')
- grad_w_out: float32 [1152, 1152], P('inner', 'dp')
- grad_w_up: float32 [1152, 4608], P('inner', 'dp')
- grad_w_down: float32 [4608, 1152], P('inner', 'dp')
- grad_bias_rows: float32 [16, 63], replicated
- grad_bias_cols: float32 [16, 63], replicated
The draws below stay inside these ranges and needn't reach their ends.
Inputs may be any that keep to these rules, and one draw needn't show every extreme that they name: Each row holds an image's grid height and width, each at most 32, whose product lies between 192 and 320; some image has exactly 320 patches.
All inputs are finite; a program needn't handle non-finite values.
Results may differ from the reference program's by a relative error of at most 0.015.
Values may be sent and summed in bfloat16 or wider, within the bound.
A program may use at most 256 MiB of HBM per device.

```python
import jax
import jax.numpy as jnp
import numpy as np
from jax import lax

D = 1152
HEADS = 16
HD = 72
FF = 4608
GS = 32
LMIN = 192
LMAX = 320
IMG_DEV = 1
IMAGES = 32
N_INNER = 4


def draw_grid(key, part):
    entries = [(grid_height, grid_width) for grid_height in range(1, GS + 1) for grid_width in range(1, GS + 1) if LMIN <= grid_height * grid_width <= LMAX]
    table = jnp.array(np.array(entries, dtype=np.int32))
    fullest = [position for position, entry in enumerate(entries) if entry[0] * entry[1] == LMAX][0]
    shortest = (LMIN + GS - 1) // GS
    tallest = entries.index((GS, shortest))
    widest = entries.index((shortest, GS))
    chosen = jax.random.randint(jax.random.fold_in(key, 11), (IMAGES,), 0, len(entries))
    anchor = jax.random.randint(jax.random.fold_in(key, 12), (), 0, IMAGES)
    chosen = chosen.at[anchor].set(fullest)
    chosen = chosen.at[(anchor + 1) % IMAGES].set(tallest)
    chosen = chosen.at[(anchor + 2) % IMAGES].set(widest)
    return table[chosen]


def block_scale(rng, shape, cuts, least, high):
    level, own = 1.0, jax.random.fold_in(rng, 6)
    for dim, parts in cuts:
        steps = jnp.exp(jax.random.uniform(jax.random.fold_in(own, dim), (parts,), jnp.float32, least / len(cuts), high / len(cuts)))
        level = level * jnp.repeat(steps, shape[dim] // parts).reshape([-1 if axis == dim else 1 for axis in range(len(shape))])
    return level


def centred(key, shape, scale, bound, shards=(), held_as=jnp.bfloat16):
    values = scale * jax.random.normal(key, shape, jnp.float32)
    if shards:
        values = values * block_scale(key, shape, shards, -0.22, 0.18)
    return jnp.clip(values, -bound, bound).astype(held_as)


def setup_inputs(seed: int = 0) -> dict:
    key_list = jax.random.split(jax.random.key(seed), 17)
    return {
        "tokens": centred(key_list[0], (IMAGES, LMAX, D), 1.0, 6.0, ((0, 32),)),
        "time_vec": centred(key_list[1], (IMAGES, D), 1.0, 6.0, ((0, 32),)),
        "grid": draw_grid(jax.random.fold_in(key_list[16], 71), 0),
        "cotangent": centred(key_list[3], (IMAGES, LMAX, D), 1.0, 6.0, ((0, 32),)),
        "gain_attn": jnp.clip(1.0 + 0.18 * jax.random.normal(key_list[4], (D,), jnp.float32), 0.1, 1.9),
        "gain_mlp": jnp.clip(1.0 + 0.18 * jax.random.normal(key_list[5], (D,), jnp.float32), 0.1, 1.9),
        "w_query": centred(key_list[6], (D, D), D ** -0.5, 0.1875, ((0, 4), (1, 8))),
        "w_key": centred(key_list[7], (D, D), D ** -0.5, 0.1875, ((0, 4), (1, 8))),
        "w_value": centred(key_list[8], (D, D), D ** -0.5, 0.1875, ((0, 4), (1, 8))),
        "w_time_query": centred(key_list[9], (D, D), D ** -0.5, 0.1875, ((0, 4), (1, 8))),
        "w_time_value": centred(key_list[10], (D, D), D ** -0.5, 0.1875, ((0, 4), (1, 8))),
        "w_out": centred(key_list[11], (D, D), (D // 32) ** -0.5, 1.0, ((0, 4), (1, 8))),
        "w_up": centred(key_list[12], (D, FF), D ** -0.5, 0.1875, ((0, 4), (1, 8))),
        "w_down": centred(key_list[13], (FF, D), FF ** -0.5, 0.09375, ((0, 4), (1, 8))),
        "bias_rows": centred(key_list[14], (HEADS, 2 * GS - 1), 0.5, 3.0, (), jnp.float32),
        "bias_cols": centred(key_list[15], (HEADS, 2 * GS - 1), 0.5, 3.0, (), jnp.float32),
    }


EPSILON = 1e-05
PRECISE = lax.Precision.HIGHEST

@jax.custom_vjp
def low(v):
    return lax.optimization_barrier(v.astype(jnp.bfloat16)).astype(jnp.float32)

@jax.custom_vjp
def low_back(v):
    return v

def low_keep(v):
    return (low(v), None)

def low_pass(kept, grad):
    return (grad,)

def back_keep(v):
    return (v, None)

def back_low(kept, grad):
    return (low(grad),)
low.defvjp(low_keep, low_pass)
low_back.defvjp(back_keep, back_low)

def layer_norm(matrix, gains):
    center = matrix - lax.optimization_barrier(jnp.mean(matrix, axis=-1, keepdims=True))
    spread = lax.optimization_barrier(jnp.mean(center * center, axis=-1, keepdims=True))
    return center * lax.rsqrt(spread + EPSILON) * gains

def slot_positions(grid, slots):
    heights = grid[:, 0]
    widths = grid[:, 1]
    length = heights * widths
    places = jnp.arange(slots, dtype=jnp.int32)
    usable = places[None, :] < length[:, None]
    clipped = jnp.minimum(places[None, :], length[:, None] - 1)
    return (usable, clipped // widths[:, None], clipped % widths[:, None])

def forward_group(params, inputs, times, grid):
    gain_attn, gain_mlp, w_query, w_key, w_value, w_time_query, w_time_value, w_out, w_up, w_down, bias_rows, bias_cols = params
    images, slots, width = inputs.shape
    flat = inputs.reshape(images * slots, width)
    normed_attn = low(layer_norm(flat, gain_attn))
    queries = jnp.dot(normed_attn, w_query, precision=PRECISE).reshape(images, slots, width)
    queries = queries + jnp.dot(times, w_time_query, precision=PRECISE)[:, None, :]
    queries = low_back(low(queries)).reshape(images, slots, HEADS, HD)
    key_heads = low_back(low(jnp.dot(normed_attn, w_key, precision=PRECISE)))
    key_heads = key_heads.reshape(images, slots, HEADS, HD)
    value_heads = jnp.dot(normed_attn, w_value, precision=PRECISE).reshape(images, slots, width)
    value_heads = value_heads + jnp.dot(times, w_time_value, precision=PRECISE)[:, None, :]
    value_heads = low_back(low(value_heads)).reshape(images, slots, HEADS, HD)
    usable, row_place, col_place = slot_positions(grid, slots)
    row_offset = row_place[:, :, None] - row_place[:, None, :] + (GS - 1)
    col_offset = col_place[:, :, None] - col_place[:, None, :] + (GS - 1)
    position = jnp.take(bias_rows, row_offset, axis=1) + jnp.take(bias_cols, col_offset, axis=1)
    position = jnp.transpose(position, (1, 0, 2, 3))
    scores = jnp.einsum('nihe,njhe->nhij', queries, key_heads, precision=PRECISE) * HD ** (-0.5) + position
    scores = low_back(scores)
    scores = jnp.where(usable[:, None, None, :], scores, -1000000000.0)
    maxima = lax.optimization_barrier(jnp.max(scores, axis=-1, keepdims=True))
    expo = jnp.exp(scores - maxima)
    probs = expo / lax.optimization_barrier(jnp.sum(expo, axis=-1, keepdims=True))
    attended = jnp.einsum('nhij,njhe->nihe', low(probs), value_heads, precision=PRECISE)
    attended = low_back(low(attended)).reshape(images * slots, width)
    mixed = flat + low_back(jnp.dot(attended, w_out, precision=PRECISE))
    normed_mlp = low(layer_norm(mixed, gain_mlp))
    up_proj = low_back(jnp.dot(normed_mlp, w_up, precision=PRECISE))
    hidden = low(jax.nn.gelu(up_proj, approximate=True))
    result = mixed + low_back(jnp.dot(hidden, w_down, precision=PRECISE))
    keep_rows = usable.reshape(images * slots, 1)
    return jnp.where(keep_rows, result, 0.0).reshape(images, slots, width)

def reference(tokens, time_vec, grid, cotangent, gain_attn, gain_mlp, w_query, w_key, w_value, w_time_query, w_time_value, w_out, w_up, w_down, bias_rows, bias_cols):
    group = IMG_DEV * N_INNER
    rounds = IMAGES // group
    params = tuple((array.astype(jnp.float32) for array in (gain_attn, gain_mlp, w_query, w_key, w_value, w_time_query, w_time_value, w_out, w_up, w_down, bias_rows, bias_cols)))
    inputs_all = tokens.astype(jnp.float32).reshape(rounds, group, LMAX, D)
    times_all = time_vec.astype(jnp.float32).reshape(rounds, group, D)
    grids_all = grid.reshape(rounds, group, 2)

    def whole(inputs_all, params):

        def advance(carry, pieces):
            return (carry, jax.checkpoint(forward_group)(params, pieces[0], pieces[1], pieces[2]))
        return lax.scan(advance, None, (inputs_all, times_all, grids_all))[1]
    output, backward = jax.vjp(whole, inputs_all, params)
    upstream = cotangent.astype(jnp.float32).reshape(rounds, group, LMAX, D)
    grad_inputs, grad_params = backward(upstream)
    return (output.reshape(IMAGES, LMAX, D).astype(jnp.bfloat16), grad_inputs.reshape(IMAGES, LMAX, D).astype(jnp.bfloat16), grad_params[0], grad_params[1], grad_params[2], grad_params[3], grad_params[4], grad_params[5], grad_params[6], grad_params[7], grad_params[8], grad_params[9], grad_params[10], grad_params[11])
```

```python
from functools import partial

import jax
import jax.numpy as jnp
from jax import lax
from jax.experimental import pallas as pl
from jax.experimental.pallas import tpu as pltpu
from jax.sharding import PartitionSpec as P

GS = 32
EPSILON = 1e-05
PRECISE = lax.Precision.HIGHEST
MESH = pl.DeviceIdType.MESH
AXES = ("dp", "inner")
SPOTS = 8


def place():
    dp, inner = lax.axis_index("dp"), lax.axis_index("inner")
    z, y = dp // 2, dp % 2
    return inner // 2, inner % 2, z + y * (7 - 2 * z)


def owner(x, core, spot):
    y = spot // 4
    z = spot + y * (7 - 2 * spot)
    return z * 2 + y, x * 2 + core


def ship(src, dst, send_sem, recv_sem, target):
    return pltpu.make_async_remote_copy(
        src_ref=src, dst_ref=dst, send_sem=send_sem, recv_sem=recv_sem, device_id=target, device_id_type=MESH
    )


def arrive(ref, sem):
    pltpu.make_async_copy(ref, ref, sem).wait()


def peers():
    x, core, spot = place()
    turn = 1 - 2 * core
    return (
        owner(x, core, (spot + turn + 8) % 8),
        owner(x, core, (spot - turn + 8) % 8),
        owner(1 - x, core, spot),
        owner(x, 1 - core, spot),
    )


def greet():
    barrier = pltpu.get_barrier_semaphore()
    for target in peers():
        pl.semaphore_signal(barrier, inc=1, device_id=target, device_id_type=MESH)
    pl.semaphore_wait(barrier, 4)


def every(count, body):
    def step(k, carry):
        body(k)
        return carry

    lax.fori_loop(0, count, step, 0)


class Gather:
    def __init__(self, home, pieces, early, ring_send, ring_recv, side_send, side_recv, pair_send, pair_recv):
        self.home, self.pieces, self.early = home, pieces, early
        self.ring, self.side, self.pair = (ring_send, ring_recv), (side_send, side_recv), (pair_send, pair_recv)
        self.x, self.core, self.spot = place()
        self.turn = 1 - 2 * self.core
        self.next, unused, self.across, self.partner = peers()

    @staticmethod
    def semaphores(pieces, early):
        dma = pltpu.SemaphoreType.DMA
        shapes = ((SPOTS - 1, pieces + early), (SPOTS, pieces), (SPOTS, 2 * pieces))
        return [dma(shape) for shape in shapes for twice in range(2)]

    def sent(self, pair, ref, slot, target):
        return ship(ref, ref, pair[0].at[slot], pair[1].at[slot], target)

    def who(self, step, plane):
        source = (self.spot - self.turn * step + 16) % 8
        return owner(self.x if plane == 0 else 1 - self.x, self.core, source)

    def step(self, step):
        for k in range(self.pieces):
            ref = self.home(k, self.who(step, 0))

            @pl.when(step > 0)
            def _():
                arrive(ref, self.ring[1].at[step - 1, k])

            @pl.when(step < SPOTS - 1)
            def _():
                self.sent(self.ring, ref, (step, k), self.next).start()

            if k >= self.early:
                self.sent(self.side, ref, (step, k), self.across).start()
            else:

                @pl.when(step == 0)
                def _():
                    self.sent(self.side, ref, (step, k), self.across).start()

            self.sent(self.pair, ref, (step, k), self.partner).start()
        for k in range(self.early):
            ref = self.home(k, self.who(step, 1))

            @pl.when(step == 0)
            def _():
                arrive(ref, self.side[1].at[step, k])

            @pl.when(step > 0)
            def _():
                arrive(ref, self.ring[1].at[step - 1, self.pieces + k])

            @pl.when(step < SPOTS - 1)
            def _():
                self.sent(self.ring, ref, (step, self.pieces + k), self.next).start()

            self.sent(self.pair, ref, (step, self.pieces + k), self.partner).start()

        @pl.when(step > 0)
        def _():
            self.crossed(step - 1)

    def crossed(self, step):
        for k in range(self.early, self.pieces):
            ref = self.home(k, self.who(step, 1))
            arrive(ref, self.side[1].at[step, k])
            self.sent(self.pair, ref, (step, self.pieces + k), self.partner).start()

    def finish(self):
        self.crossed(SPOTS - 1)

        def last(step):
            source = (self.spot + self.turn * step + 16) % 8
            for plane in range(2):
                who = owner(self.x if plane == 0 else 1 - self.x, 1 - self.core, source)
                for k in range(self.pieces):
                    arrive(self.home(k, who), self.pair[1].at[step, plane * self.pieces + k])
                    mine = self.home(k, self.who(step, plane))
                    self.sent(self.pair, mine, (step, plane * self.pieces + k), self.partner).wait_send()
            for k in range(self.pieces):
                ref = self.home(k, self.who(step, 0))

                @pl.when(step < SPOTS - 1)
                def _():
                    self.sent(self.ring, ref, (step, k), self.next).wait_send()

                if k >= self.early:
                    self.sent(self.side, ref, (step, k), self.across).wait_send()
                else:

                    @pl.when(step == 0)
                    def _():
                        self.sent(self.side, ref, (step, k), self.across).wait_send()

            for k in range(self.early):
                ref = self.home(k, self.who(step, 1))

                @pl.when(step < SPOTS - 1)
                def _():
                    self.sent(self.ring, ref, (step, self.pieces + k), self.next).wait_send()

        every(SPOTS, last)


def keep_own(refs, sem):
    copies = [pltpu.make_async_copy(src, dst, sem.at[k]) for k, (src, dst) in enumerate(refs)]
    for copy in copies:
        copy.start()
    for copy in copies:
        copy.wait()


def attention_gather_kernel(
    early, block, times, w_times, small_out, times_out, terms_out, time_buf, turned, own_sem, time_send, time_recv,
    term_send, term_recv, *sems,
):
    x, core, spot = place()
    me = owner(x, core, spot)
    here = me[0] * 4 + me[1]
    rows = block.shape[0]
    barrier = pltpu.get_barrier_semaphore()

    def other(k):
        place_of = (here + k) % 32
        return place_of, (place_of // 4, place_of % 4)

    def signal(k):
        pl.semaphore_signal(barrier, inc=1, device_id=other(k + 1)[1], device_id_type=MESH)

    every(31, signal)
    pl.semaphore_wait(barrier, 31)

    def home(k, who):
        lo, size = ((0, early), (early, rows - early))[k]
        return small_out.at[who[1], pl.ds(who[0] * rows + lo, size), :]

    def time_copy(k):
        there, target = other(k + 1)
        return ship(times.at[target[1]], time_buf.at[here], time_send.at[k], time_recv.at[k], target)

    def term_copy(k):
        there, target = other(k + 1)
        return ship(turned.at[there], terms_out.at[here], term_send.at[k], term_recv.at[k], target)

    every(31, lambda k: time_copy(k).start())
    time_buf[here] = times[me[1]]
    gather = Gather(home, 2, 1, *sems)
    keep_own([(block.at[pl.ds(0, early), :], home(0, me)), (block.at[pl.ds(early, rows - early), :], home(1, me))], own_sem)
    gather.step(0)
    every(31, lambda k: arrive(time_buf.at[(here + 31 - k) % 32], time_recv.at[k]))
    known = time_buf[...].reshape(32, time_buf.shape[2])
    times_out[...] = known
    terms = jnp.dot(known.astype(jnp.bfloat16), w_times[...], preferred_element_type=jnp.float32)
    turned[...] = terms.reshape(32, 1, terms.shape[1])
    every(31, lambda k: term_copy(k).start())
    terms_out[here] = turned[here]
    every(SPOTS - 1, lambda k: gather.step(k + 1))
    every(31, lambda k: arrive(terms_out.at[(here + 31 - k) % 32], term_recv.at[k]))

    def sent(k):
        time_copy(k).wait_send()
        term_copy(k).wait_send()

    every(31, sent)
    gather.finish()


def attention_gather(block, times, w_times):
    rows, width = block.shape
    early = rows * 4 // 9
    lanes = times.shape[2]
    dma = pltpu.SemaphoreType.DMA
    vmem = pl.BlockSpec(memory_space=pltpu.VMEM)
    return pl.pallas_call(
        partial(attention_gather_kernel, early),
        out_shape=(
            jax.ShapeDtypeStruct((4, SPOTS * rows, width), block.dtype),
            jax.ShapeDtypeStruct((32, lanes), jnp.float32),
            jax.ShapeDtypeStruct((32, 1, w_times.shape[1]), jnp.float32),
        ),
        in_specs=[vmem] * 3,
        out_specs=(pl.BlockSpec(memory_space=pl.ANY), vmem, vmem),
        scratch_shapes=[
            pltpu.VMEM((32, 1, lanes), jnp.float32),
            pltpu.VMEM((32, 1, w_times.shape[1]), jnp.float32),
            dma((2,)),
            dma((31,)),
            dma((31,)),
            dma((31,)),
            dma((31,)),
            *Gather.semaphores(2, 1),
        ],
        compiler_params=pltpu.CompilerParams(collective_id=0, has_side_effects=True),
        name="attention_gather",
    )(block, times, w_times)


def nt(a, b):
    return lax.dot_general(a, b, (((1,), (1,)), ((), ())), preferred_element_type=jnp.float32)


def nn(a, b):
    return lax.dot_general(a, b, (((1,), (0,)), ((), ())), preferred_element_type=jnp.float32)


def tn(a, b):
    return lax.dot_general(a, b, (((0,), (0,)), ((), ())), preferred_element_type=jnp.float32)


def attention_kernel(
    early, scale, block, small_in, normed, t_query, t_value, places, hots, mask, down_out, up_out, queries, keys, values,
    probs, attended, weights, own_sem, load_sem, *sems,
):
    x, core, spot = place()
    me = owner(x, core, spot)
    rows, width = block.shape[0] // 2, block.shape[1]
    size = rows // 2
    greet()
    loads = [pltpu.make_async_copy(small_in.at[k], weights.at[k], load_sem.at[k]) for k in range(3)]
    for copy in loads:
        copy.start()

    def home(k, who):
        j, i = who
        if k == 0:
            return down_out.at[pl.ds(j * rows, early), pl.ds(i * width, width)]
        if k == 1:
            return down_out.at[pl.ds(j * rows + early, rows - early), pl.ds(i * width, width)]
        return up_out.at[pl.ds((j * 4 + i) * rows, rows), :]

    gather = Gather(home, 3, 1, *sems)
    bounds = ((0, early), (early, rows - early), (rows, rows))
    keep_own([(block.at[pl.ds(*bounds[k]), :], home(k, me)) for k in range(3)], own_sem)

    def heads(p):
        known = normed[...]
        at = pl.ds(pl.multiple_of(p * rows, 16), rows)
        query = (nt(known, weights[0, at, :]) + t_query[p]).astype(jnp.bfloat16)
        key = nt(known, weights[1, at, :]).astype(jnp.bfloat16)
        value = (nt(known, weights[2, at, :]) + t_value[p]).astype(jnp.bfloat16)
        queries[p] = query
        keys[p] = key
        values[p] = value
        outs = []
        for t in range(2):
            part = slice(t * size, (t + 1) * size)
            scores = (nt(query[:, part], key[:, part]) + nt(places[2 * p + t], hots[...])) * scale
            scores = jnp.where(mask[...] > 0.0, scores, -1000000000.0)
            expo = jnp.exp(scores - jnp.max(scores, axis=-1, keepdims=True))
            low = (expo / jnp.sum(expo, axis=-1, keepdims=True)).astype(jnp.bfloat16)
            probs[2 * p + t] = low
            outs.append(nn(low, value[:, part]))
        attended[p] = jnp.concatenate(outs, axis=1).astype(jnp.bfloat16)

    def work(step):
        gather.step(step)

        @pl.when(step == 0)
        def _():
            for copy in loads:
                copy.wait()

        heads(step)

    every(SPOTS, work)
    gather.finish()


def attention_forward(block, small, normed, t_query, t_value, places, hots, mask, scale):
    rows, width = block.shape[0] // 2, block.shape[1]
    early = rows * 8 // 9
    slots = normed.shape[0]
    dma = pltpu.SemaphoreType.DMA
    vmem, far = pl.BlockSpec(memory_space=pltpu.VMEM), pl.BlockSpec(memory_space=pl.ANY)
    low = block.dtype
    pair = jax.ShapeDtypeStruct((SPOTS, slots, rows), low)
    return pl.pallas_call(
        partial(attention_kernel, early, scale),
        out_shape=(
            jax.ShapeDtypeStruct((SPOTS * rows, 4 * width), low),
            jax.ShapeDtypeStruct((32 * rows, width), low),
            pair,
            pair,
            pair,
            jax.ShapeDtypeStruct((2 * SPOTS, slots, slots), low),
            pair,
        ),
        in_specs=[vmem, far] + [vmem] * 6,
        out_specs=(far, far) + (vmem,) * 5,
        scratch_shapes=[
            pltpu.VMEM((3, SPOTS * rows, width), low),
            dma((3,)),
            dma((3,)),
            *Gather.semaphores(3, 1),
        ],
        compiler_params=pltpu.CompilerParams(collective_id=1, has_side_effects=True, vmem_limit_bytes=60 << 20),
        name="attention_forward",
    )(block, small, normed, t_query, t_value, places, hots, mask)


def pile(target, sources, size):
    tile = 16

    def body(k):
        total = None
        for ref, base in sources:
            piece = ref[pl.ds(pl.multiple_of(base + k * tile, 16), tile), :].astype(jnp.float32)
            total = piece if total is None else total + piece
        ref, base = target
        ref[pl.ds(pl.multiple_of(base + k * tile, 16), tile), :] = total.astype(ref.dtype)

    every(size // tile, body)


class Scatter:
    def __init__(
        self, home, parts, rows, early, result, pair_buf, ring_buf, side_buf, last_buf, own_buf, own_sem, ring_send,
        ring_recv, side_send, side_recv, last_send, last_recv, pair_send, pair_recv,
    ):
        self.home, self.parts, self.rows, self.early = home, parts, rows, early
        self.block = parts * rows
        self.result = result
        self.pair_buf, self.ring_buf, self.side_buf, self.last_buf, self.own_buf = (
            pair_buf, ring_buf, side_buf, last_buf, own_buf,
        )
        self.own_sem = own_sem
        self.ring, self.side, self.pair = (ring_send, ring_recv), (side_send, side_recv), (pair_send, pair_recv)
        self.last = (last_send, last_recv)
        self.x, self.core, self.spot = place()
        self.turn = 1 - 2 * self.core
        self.next, unused, self.across, self.partner = peers()

    @staticmethod
    def scratch(parts, rows, early, width, low):
        dma = pltpu.SemaphoreType.DMA
        block = parts * rows
        return [
            pltpu.VMEM((SPOTS, 2, block, width), low),
            pltpu.VMEM((SPOTS - 1, block + early, width), low),
            pltpu.VMEM((SPOTS, block - early, width), low),
            pltpu.VMEM((early, width), low),
            pltpu.VMEM((2, 2, block, width), low),
            dma((2, 2, parts)),
            dma((SPOTS - 1, 3)),
            dma((SPOTS - 1, 3)),
            dma((SPOTS,)),
            dma((SPOTS,)),
            dma((1,)),
            dma((1,)),
            dma((SPOTS, 2, parts)),
            dma((SPOTS, 2, parts)),
        ]

    def span(self, part):
        return pl.ds(part * self.rows, self.rows)

    def pair_copy(self, step, plane, part):
        goal = (self.spot + self.turn * (1 + step) + 16) % 8
        who = owner(self.x if plane == 0 else 1 - self.x, 1 - self.core, goal)
        return ship(
            self.home(part, who),
            self.pair_buf.at[step, plane, self.span(part), :],
            self.pair[0].at[step, plane, part],
            self.pair[1].at[step, plane, part],
            self.partner,
        )

    def begin(self):
        def give(step):
            for plane in (1, 0):
                for part in range(self.parts):
                    self.pair_copy(step, plane, part).start()

        every(SPOTS, give)
        self.fetch(0)

    def loads(self, step, plane):
        goal = (self.spot - self.turn * (1 + step) + 16) % 8
        who = owner(self.x if plane == 0 else 1 - self.x, self.core, goal)
        return [
            pltpu.make_async_copy(
                self.home(part, who),
                self.own_buf.at[step % 2, plane, self.span(part), :],
                self.own_sem.at[step % 2, plane, part],
            )
            for part in range(self.parts)
        ]

    def fetch(self, step):
        for plane in (1, 0):
            for copy in self.loads(step, plane):
                copy.start()

    def ready(self, step, plane):
        for copy in self.loads(step, plane):
            copy.wait()
        for part in range(self.parts):
            arrive(self.pair_buf.at[step, plane, self.span(part), :], self.pair[1].at[step, plane, part])

    def side_copy(self, step):
        src = self.pair_buf.at[step, 1, pl.ds(self.early, self.block - self.early), :]
        return ship(src, self.side_buf.at[step], self.side[0].at[step], self.side[1].at[step], self.across)

    def lane(self, n):
        return (
            (0, 0, 0, self.early),
            (0, self.early, self.early, self.block - self.early),
            (1, 0, self.block, self.early),
        )[n]

    def ring_copy(self, step, n):
        plane, lo, base, size = self.lane(n)
        return ship(
            self.pair_buf.at[step, plane, pl.ds(lo, size), :],
            self.ring_buf.at[step, pl.ds(base, size), :],
            self.ring[0].at[step, n],
            self.ring[1].at[step, n],
            self.next,
        )

    def sources(self, step, n, ring):
        plane, lo, base, size = self.lane(n)
        refs = [(self.own_buf.at[step % 2, plane], lo), (self.pair_buf.at[step, plane], lo)]
        if n == 1:
            refs.append((self.side_buf.at[step], 0))
        if ring:
            refs.append((self.ring_buf.at[step - 1], base))
        return refs

    def across_part(self, step):
        self.ready(step, 1)
        held = self.pair_buf.at[step, 1]
        mine = self.own_buf.at[step % 2, 1]
        pile((held, self.early), [(mine, self.early), (held, self.early)], self.block - self.early)
        self.side_copy(step).start()
        self.ready(step, 0)

    def step(self, step):
        self.across_part(step)
        self.fetch(step + 1)
        for n in range(3):
            plane, lo, base, size = self.lane(n)
            if n == 1:
                arrive(self.side_buf.at[step], self.side[1].at[step])

            @pl.when(step == 0)
            def _():
                pile((self.pair_buf.at[step, plane], lo), self.sources(step, n, False), size)

            @pl.when(step > 0)
            def _():
                arrive(self.ring_buf.at[step - 1, pl.ds(base, size), :], self.ring[1].at[step - 1, n])
                pile((self.pair_buf.at[step, plane], lo), self.sources(step, n, True), size)

            self.ring_copy(step, n).start()

    def finish(self):
        step = SPOTS - 1
        self.across_part(step)
        for n in (2, 1, 0):
            plane, lo, base, size = self.lane(n)
            arrive(self.ring_buf.at[step - 1, pl.ds(base, size), :], self.ring[1].at[step - 1, n])
            refs = self.sources(step, n, True)
            if n == 2:
                pile((self.pair_buf.at[step, 1], 0), refs, size)
                src = self.pair_buf.at[step, 1, pl.ds(0, size), :]
                over = ship(src, self.last_buf, self.last[0].at[0], self.last[1].at[0], self.across)
                over.start()
                continue
            if n == 1:
                arrive(self.side_buf.at[step], self.side[1].at[step])
            else:
                arrive(self.last_buf, self.last[1].at[0])
                refs.append((self.last_buf, 0))
            pile((self.result, lo), refs, size)
        over.wait_send()

        def sent(step):
            for plane in range(2):
                for part in range(self.parts):
                    self.pair_copy(step, plane, part).wait_send()
            self.side_copy(step).wait_send()

            @pl.when(step < SPOTS - 1)
            def _():
                for n in range(3):
                    self.ring_copy(step, n).wait_send()

        every(SPOTS, sent)


def backward_kernel(
    early, scale, down_in, up_in, small_in, normed, grad_attended, queries, keys, values, probs, hots, result, small_out,
    grad_normed, squares, sums, weights, load_sem, grads, grad_sem, *scratch,
):
    rows, width = result.shape[0] // 2, result.shape[1]
    size = rows // 2
    sides = hots.shape[1]
    greet()
    loads = [pltpu.make_async_copy(small_in.at[k], weights.at[k], load_sem.at[k]) for k in range(3)]
    for copy in loads:
        copy.start()

    def home(part, who):
        j, i = who
        if part == 0:
            return down_in.at[pl.ds(j * rows, rows), pl.ds(i * width, width)]
        return up_in.at[pl.ds((j * 4 + i) * rows, rows), :]

    scatter = Scatter(home, 2, rows, early, result, *scratch)
    scatter.begin()
    grad_normed[...] = jnp.zeros_like(grad_normed)

    def keep(p, k):
        return pltpu.make_async_copy(
            grads.at[p % 2, k], small_out.at[k, pl.ds(pl.multiple_of(p * rows, 16), rows), :], grad_sem.at[p % 2, k]
        )

    def heads(p):
        query, key, value, above = queries[p], keys[p], values[p], grad_attended[p]
        hot = hots[...]
        parts = ([], [], [])
        for t in range(2):
            part = slice(t * size, (t + 1) * size)
            low = probs[2 * p + t]
            wide = low.astype(jnp.float32)
            grad_probs = nt(above[:, part], value[:, part])
            inner = jnp.sum(wide * grad_probs, axis=-1, keepdims=True)
            grad_scores = (wide * (grad_probs - inner)).astype(jnp.bfloat16)
            parts[0].append(nn(grad_scores, key[:, part]) * scale)
            parts[1].append(tn(grad_scores, query[:, part]) * scale)
            parts[2].append(tn(low, above[:, part]))
            across = nn(grad_scores, hot)
            high = across.astype(jnp.bfloat16)
            rest = (across - high.astype(jnp.float32)).astype(jnp.bfloat16)
            squares[2 * p + t] = tn(hot, high) + tn(hot, rest)

        @pl.when(p >= 2)
        def _():
            for k in range(3):
                keep(p - 2, k).wait()

        known = normed[...]
        at = pl.ds(pl.multiple_of(p * rows, 16), rows)
        total = None
        for k in range(3):
            grad = jnp.concatenate(parts[k], axis=1).astype(jnp.bfloat16)
            sums[k, p] = jnp.sum(grad.astype(jnp.float32), axis=0, keepdims=True)
            grads[p % 2, k] = tn(grad, known).astype(jnp.bfloat16)
            keep(p, k).start()
            term = nn(grad, weights[k, at, :])
            total = term if total is None else total + term
        grad_normed[...] += total

    def work(step):
        @pl.when(step < SPOTS - 1)
        def _():
            scatter.step(step)

        @pl.when(step == 0)
        def _():
            for copy in loads:
                copy.wait()

        heads(step)

    every(SPOTS, work)
    for p in (SPOTS - 2, SPOTS - 1):
        for k in range(3):
            keep(p, k).wait()
    scatter.finish()


def attention_backward(down, up, small, normed, grad_attended, queries, keys, values, probs, hots, scale):
    rows, width = up.shape[0] // 32, up.shape[1]
    early = rows * 8 // 9
    slots = normed.shape[0]
    sides = hots.shape[1]
    low = up.dtype
    dma = pltpu.SemaphoreType.DMA
    vmem, far = pl.BlockSpec(memory_space=pltpu.VMEM), pl.BlockSpec(memory_space=pl.ANY)
    return pl.pallas_call(
        partial(backward_kernel, early, scale),
        out_shape=(
            jax.ShapeDtypeStruct((2 * rows, width), jnp.float32),
            jax.ShapeDtypeStruct((3, SPOTS * rows, width), low),
            jax.ShapeDtypeStruct((slots, width), jnp.float32),
            jax.ShapeDtypeStruct((2 * SPOTS, sides, sides), jnp.float32),
            jax.ShapeDtypeStruct((3, SPOTS, 1, rows), jnp.float32),
        ),
        in_specs=[far] * 3 + [vmem] * 7,
        out_specs=(vmem, far, vmem, vmem, vmem),
        scratch_shapes=[
            pltpu.VMEM((3, SPOTS * rows, width), low),
            dma((3,)),
            pltpu.VMEM((2, 3, rows, width), low),
            dma((2, 3)),
            *Scatter.scratch(2, rows, early, width, low),
        ],
        compiler_params=pltpu.CompilerParams(collective_id=2, has_side_effects=True, vmem_limit_bytes=63 << 20),
        name="attention_backward",
    )(down, up, small, normed, grad_attended, queries, keys, values, probs, hots)


def last_sums_kernel(early, small_in, out_in, extra_in, result, extra_out, own_sem, note_sems, scratch):
    x, core, spot = place()
    rows = result.shape[0]
    greet()

    def home(part, who):
        return small_in.at[who[1], pl.ds(who[0] * rows, rows), :]

    def note(k, who):
        return extra_out.at[who[0] * 4 + who[1]]

    scatter = Scatter(home, 1, rows, early, result, *scratch)
    scatter.begin()
    notes = Gather(note, 1, 1, *note_sems)
    keep_own([(extra_in, note(0, owner(x, core, spot)))], own_sem)

    def work(step):
        notes.step(step)

        @pl.when(step < SPOTS - 1)
        def _():
            scatter.step(step)

    every(SPOTS, work)
    scatter.finish()
    notes.finish()


def last_sums(small, extra):
    rows, width = small.shape[1] // SPOTS, small.shape[2]
    early = rows * 4 // 9
    low = small.dtype
    vmem, far = pl.BlockSpec(memory_space=pltpu.VMEM), pl.BlockSpec(memory_space=pl.ANY)

    def kernel(small_in, extra_in, result, extra_out, own_sem, *rest):
        last_sums_kernel(early, small_in, None, extra_in, result, extra_out, own_sem, rest[:6], rest[6:])

    return pl.pallas_call(
        kernel,
        out_shape=(
            jax.ShapeDtypeStruct((rows, width), jnp.float32),
            jax.ShapeDtypeStruct((32, *extra.shape), extra.dtype),
        ),
        in_specs=[far, vmem],
        out_specs=(vmem, vmem),
        scratch_shapes=[
            pltpu.SemaphoreType.DMA((1,)),
            *Gather.semaphores(1, 1),
            *Scatter.scratch(1, rows, early, width, low),
        ],
        compiler_params=pltpu.CompilerParams(collective_id=3, has_side_effects=True),
        name="last_sums",
    )(small, extra)


def layer_norm(matrix, gains):
    center = matrix - jnp.mean(matrix, axis=-1, keepdims=True)
    spread = jnp.mean(center * center, axis=-1, keepdims=True)
    return center * lax.rsqrt(spread + EPSILON) * gains


def slot_positions(grid, slots):
    heights = grid[:, 0]
    widths = grid[:, 1]
    length = heights * widths
    places = jnp.arange(slots, dtype=jnp.int32)
    usable = places[None, :] < length[:, None]
    clipped = jnp.minimum(places[None, :], length[:, None] - 1)
    return (usable, clipped // widths[:, None], clipped % widths[:, None])


def offset_table():
    shape = (GS, GS, 2 * GS - 1)
    source = lax.broadcasted_iota(jnp.int32, shape, 0)
    target = lax.broadcasted_iota(jnp.int32, shape, 1)
    offset = lax.broadcasted_iota(jnp.int32, shape, 2)
    return (source - target + (GS - 1) == offset).astype(jnp.float32)


def side_hot(places):
    sides = lax.broadcasted_iota(jnp.int32, (1, 1, GS), 2)
    return (places[:, :, None] == sides).astype(jnp.float32)


def position_bias(row_hot, col_hot, bias_rows, bias_cols, offset_hot):
    terms = []
    for hot_side, table in ((row_hot, bias_rows), (col_hot, bias_cols)):
        square = jnp.einsum("hd,rsd->hrs", table, offset_hot, precision=PRECISE)
        partial_rows = jnp.einsum("nir,hrs->nhis", hot_side, square, precision=PRECISE)
        terms.append(jnp.einsum("nhis,njs->nhij", partial_rows, hot_side, precision=PRECISE))
    return terms[0] + terms[1]


def bias_grads(grad_scores, row_hot, col_hot, offset_hot):
    results = []
    for hot_side in (row_hot, col_hot):
        partial_cols = jnp.einsum("nhij,njs->nhis", grad_scores, hot_side, precision=PRECISE)
        square = jnp.einsum("nir,nhis->hrs", hot_side, partial_cols, precision=PRECISE)
        results.append(jnp.einsum("hrs,rsd->hd", square, offset_hot, precision=PRECISE))
    return (results[0], results[1])


def masked_scores(queries, key_heads, position, usable):
    head_size = queries.shape[3]
    raw = jnp.einsum("nihe,njhe->nhij", queries, key_heads, preferred_element_type=jnp.float32)
    scores = raw * head_size ** (-0.5) + position
    return jnp.where(usable[:, None, None, :], scores, -1000000000.0)


def layer(tokens, grid, cotangent, gain_attn, gain_mlp, bias_rows, bias_cols, turned, time_query, time_value):
    images, slots, width = tokens.shape
    heads = bias_rows.shape[0]
    head_size = width // heads
    scale = head_size ** (-0.5)
    flat = images * slots
    gelu_tanh = partial(jax.nn.gelu, approximate=True)
    t_query, t_key, t_value, t_out, t_down, t_up = turned
    ahead = partial(jnp.einsum, "rd,ed->re", preferred_element_type=jnp.float32)
    back = partial(jnp.einsum, "re,ed->rd", preferred_element_type=jnp.float32)

    def outer(grads, values):
        return jnp.einsum("re,rd->ed", grads, values, preferred_element_type=jnp.float32).astype(jnp.bfloat16)

    inputs = tokens.astype(jnp.float32).reshape(flat, width)
    normed_attn = layer_norm(inputs, gain_attn).astype(jnp.bfloat16)
    shape = (images, slots, heads, head_size)
    queries = ahead(normed_attn, t_query).reshape(images, slots, width)
    queries = (queries + time_query[:, None, :]).astype(jnp.bfloat16).reshape(shape)
    key_heads = ahead(normed_attn, t_key).astype(jnp.bfloat16).reshape(shape)
    value_heads = ahead(normed_attn, t_value).reshape(images, slots, width)
    value_heads = (value_heads + time_value[:, None, :]).astype(jnp.bfloat16).reshape(shape)
    usable, row_place, col_place = slot_positions(grid, slots)
    offset_hot = offset_table()
    row_hot = side_hot(row_place)
    col_hot = side_hot(col_place)
    position = position_bias(row_hot, col_hot, bias_rows, bias_cols, offset_hot)
    scores = masked_scores(queries, key_heads, position, usable)
    maxima = jnp.max(scores, axis=-1, keepdims=True)
    expo = jnp.exp(scores - maxima)
    totals = jnp.sum(expo, axis=-1, keepdims=True)
    probs_low = (expo / totals).astype(jnp.bfloat16)
    attended = jnp.einsum("nhij,njhe->nihe", probs_low, value_heads, preferred_element_type=jnp.float32)
    attended = attended.astype(jnp.bfloat16).reshape(flat, width)
    mixed = inputs + ahead(attended, t_out)
    normed_mlp = layer_norm(mixed, gain_mlp).astype(jnp.bfloat16)
    up_proj = ahead(normed_mlp, t_up)
    hidden = gelu_tanh(up_proj).astype(jnp.bfloat16)
    keep_rows = usable.reshape(flat, 1)
    result = jnp.where(keep_rows, mixed + ahead(hidden, t_down), 0.0)
    output = result.astype(jnp.bfloat16).reshape(images, slots, width)
    upstream = jnp.where(keep_rows, cotangent.astype(jnp.float32).reshape(flat, width), 0.0)
    upstream_low = upstream.astype(jnp.bfloat16)
    grad_down = outer(upstream_low, hidden)
    grad_hidden = back(upstream_low, t_down)
    unused_gelu, gelu_back = jax.vjp(gelu_tanh, up_proj)
    grad_up_proj = gelu_back(grad_hidden)[0].astype(jnp.bfloat16)
    grad_up = outer(grad_up_proj, normed_mlp)
    grad_normed_mlp = back(grad_up_proj, t_up)
    unused_mlp, norm_mlp_back = jax.vjp(layer_norm, mixed, gain_mlp)
    grad_mixed_norm, grad_gain_mlp = norm_mlp_back(grad_normed_mlp)
    grad_mixed = upstream + grad_mixed_norm
    grad_mixed_low = grad_mixed.astype(jnp.bfloat16)
    grad_out = outer(grad_mixed_low, attended)
    grad_attended = back(grad_mixed_low, t_out).astype(jnp.bfloat16).reshape(shape)
    scores = masked_scores(queries, key_heads, position, usable)
    probs = jnp.exp(scores - maxima) / totals
    probs_low = probs.astype(jnp.bfloat16)
    grad_probs = jnp.einsum("nihe,njhe->nhij", grad_attended, value_heads, preferred_element_type=jnp.float32)
    inner_sum = jnp.sum(probs * grad_probs, axis=-1, keepdims=True)
    grad_scores = (probs * (grad_probs - inner_sum)).astype(jnp.bfloat16)
    grad_queries = jnp.einsum("nhij,njhe->nihe", grad_scores, key_heads, preferred_element_type=jnp.float32) * scale
    grad_queries = grad_queries.astype(jnp.bfloat16).reshape(images, slots, width)
    grad_keys = jnp.einsum("nhij,nihe->njhe", grad_scores, queries, preferred_element_type=jnp.float32) * scale
    grad_keys = grad_keys.astype(jnp.bfloat16).reshape(flat, width)
    grad_values = jnp.einsum("nhij,nihe->njhe", probs_low, grad_attended, preferred_element_type=jnp.float32)
    grad_values = grad_values.astype(jnp.bfloat16).reshape(images, slots, width)
    grad_rows_table, grad_cols_table = bias_grads(grad_scores.astype(jnp.float32), row_hot, col_hot, offset_hot)
    flat_queries = grad_queries.reshape(flat, width)
    flat_values = grad_values.reshape(flat, width)
    grad_query = outer(flat_queries, normed_attn)
    grad_key = outer(grad_keys, normed_attn)
    grad_value = outer(flat_values, normed_attn)
    slot_queries = jnp.sum(grad_queries.astype(jnp.float32), axis=1)
    slot_values = jnp.sum(grad_values.astype(jnp.float32), axis=1)
    grad_normed_attn = back(flat_queries, t_query) + back(grad_keys, t_key) + back(flat_values, t_value)
    unused_attn, norm_attn_back = jax.vjp(layer_norm, inputs, gain_attn)
    grad_inputs_norm, grad_gain_attn = norm_attn_back(grad_normed_attn)
    grad_tokens = (grad_mixed + grad_inputs_norm).astype(jnp.bfloat16).reshape(images, slots, width)
    return (
        output,
        grad_tokens,
        (grad_gain_attn, grad_gain_mlp, grad_rows_table, grad_cols_table, slot_queries, slot_values),
        (grad_query, grad_key, grad_value, grad_out, grad_down, grad_up),
    )


def time_terms(time_vec, w_time_query, w_time_value):
    all_times = lax.all_gather(time_vec, AXES, axis=0, tiled=True)
    rows = w_time_query.shape[0]
    mine = lax.dynamic_slice_in_dim(all_times, lax.axis_index("inner") * rows, rows, axis=1)
    both = jnp.concatenate([w_time_query, w_time_value], axis=1)
    return mine, jnp.dot(mine, both, preferred_element_type=jnp.float32)


def time_grads(mine, slot_sums, cols):
    column = lax.axis_index("dp") * cols
    picked = lax.dynamic_slice_in_dim(slot_sums, column, cols, axis=1)
    return jnp.einsum("nd,ne->de", mine.astype(jnp.float32), picked, precision=PRECISE)


def by_rings(
    tokens, time_vec, grid, cotangent, gain_attn, gain_mlp, w_query, w_key, w_value, w_time_query, w_time_value, w_out,
    w_up, w_down, bias_rows, bias_cols,
):
    images, slots, width = tokens.shape
    slab, rows = w_query.shape
    heads = bias_rows.shape[0]
    scale = (width // heads) ** (-0.5)
    gelu_tanh = partial(jax.nn.gelu, approximate=True)
    ahead = partial(jnp.einsum, "rd,ed->re", preferred_element_type=jnp.float32)
    back = partial(jnp.einsum, "re,ed->rd", preferred_element_type=jnp.float32)

    def outer(grads, values):
        return jnp.einsum("re,rd->ed", grads, values, preferred_element_type=jnp.float32).astype(jnp.bfloat16)

    small = jnp.stack([w_query.T, w_key.T, w_value.T, w_out.T])
    wide = w_up.T.reshape(4, rows, slab)
    swapped = lax.all_to_all(jnp.stack([small, wide], axis=1), "inner", 0, 0)
    joined = jnp.transpose(swapped, (1, 2, 0, 3)).reshape(2, rows, width)
    w_times = jnp.concatenate([w_time_query, w_time_value], axis=1)
    w_times = jnp.pad(w_times, ((0, -slab % 128), (0, -2 * rows % 128)))
    times = time_vec.astype(jnp.float32).reshape(4, 1, slab)
    times = jnp.pad(times, ((0, 0), (0, 0), (0, -slab % 128)))
    t_small, all_times, terms = attention_gather(joined[0], times, w_times)
    all_times = all_times[:, :slab]
    terms = terms.reshape(SPOTS, 4, -1)[:, :, : 2 * rows].sum(axis=1).reshape(SPOTS, 1, 2 * rows)

    inputs = tokens.astype(jnp.float32).reshape(slots, width)
    normed_attn = layer_norm(inputs, gain_attn).astype(jnp.bfloat16)
    usable, row_place, col_place = slot_positions(grid, slots)
    offset_hot = offset_table()
    hot = jnp.concatenate([side_hot(row_place)[0], side_hot(col_place)[0]], axis=1)
    squares = [
        jnp.einsum("hd,rsd->hrs", table, offset_hot, precision=PRECISE) for table in (bias_rows, bias_cols)
    ]
    places = jnp.concatenate(
        [
            jnp.einsum("ir,hrs->his", hot[:, GS * k : GS * (k + 1)], squares[k] / scale, precision=PRECISE)
            for k in range(2)
        ],
        axis=2,
    )
    high = lax.reduce_precision(places, 8, 7)
    places = jnp.concatenate([high, places - high], axis=2).astype(jnp.bfloat16)
    hot = hot.astype(jnp.bfloat16)
    hots = jnp.concatenate([hot, hot], axis=1)
    mask = usable.astype(jnp.float32)
    block = jnp.concatenate([w_down.T, joined[1]], axis=0)
    t_down, t_up, queries, keys, values, probs, attended = attention_forward(
        block, t_small, normed_attn, terms[:, :, :rows], terms[:, :, rows:], places, hots, mask, scale
    )
    attended = jnp.transpose(attended, (1, 0, 2)).reshape(slots, width)
    mixed = inputs + ahead(attended, t_small[3])
    normed_mlp = layer_norm(mixed, gain_mlp).astype(jnp.bfloat16)
    up_proj = ahead(normed_mlp, t_up)
    hidden = gelu_tanh(up_proj).astype(jnp.bfloat16)
    keep_rows = usable.reshape(slots, 1)
    result = jnp.where(keep_rows, mixed + ahead(hidden, t_down), 0.0)
    output = result.astype(jnp.bfloat16).reshape(images, slots, width)
    upstream = jnp.where(keep_rows, cotangent.astype(jnp.float32).reshape(slots, width), 0.0)
    upstream_low = upstream.astype(jnp.bfloat16)
    grad_down = outer(upstream_low, hidden)
    grad_hidden = back(upstream_low, t_down)
    unused_gelu, gelu_back = jax.vjp(gelu_tanh, up_proj)
    grad_up_proj = gelu_back(grad_hidden)[0].astype(jnp.bfloat16)
    grad_up = outer(grad_up_proj, normed_mlp)
    grad_normed_mlp = back(grad_up_proj, t_up)
    unused_mlp, norm_mlp_back = jax.vjp(layer_norm, mixed, gain_mlp)
    grad_mixed_norm, grad_gain_mlp = norm_mlp_back(grad_normed_mlp)
    grad_mixed = upstream + grad_mixed_norm
    grad_mixed_low = grad_mixed.astype(jnp.bfloat16)
    grad_out = outer(grad_mixed_low, attended)
    grad_attended = back(grad_mixed_low, t_small[3]).astype(jnp.bfloat16)
    grad_attended = jnp.transpose(grad_attended.reshape(slots, SPOTS, rows), (1, 0, 2))
    wide_block, small_grads, grad_normed_attn, table_squares, slot_sums = attention_backward(
        grad_down, grad_up, t_small, normed_attn, grad_attended, queries, keys, values, probs, hot, scale
    )
    unused_attn, norm_attn_back = jax.vjp(layer_norm, inputs, gain_attn)
    grad_inputs_norm, grad_gain_attn = norm_attn_back(grad_normed_attn)
    grad_tokens = (grad_mixed + grad_inputs_norm).astype(jnp.bfloat16).reshape(images, slots, width)
    tables = [
        jnp.einsum("hrs,rsd->hd", table_squares[:, cut, cut], offset_hot, precision=PRECISE)
        for cut in (slice(0, GS), slice(GS, 2 * GS))
    ]
    own = (grad_gain_attn, grad_gain_mlp, *tables, slot_sums[0], slot_sums[2])
    notes = jnp.stack([jnp.pad(value.reshape(-1), (0, width - value.size)) for value in own])
    notes = jnp.pad(notes, ((0, 2), (0, 0)))
    small_block, notes = last_sums(jnp.concatenate([small_grads, grad_out[None]], axis=0), notes)
    totals = notes[:, :4].sum(axis=0)
    entries = bias_rows.size
    table = bias_rows.shape
    joined = jnp.stack([small_block, wide_block[rows:]]).astype(jnp.bfloat16)
    parted = jnp.transpose(joined.reshape(2, rows, 4, slab), (2, 0, 1, 3))
    swapped = lax.all_to_all(parted, "inner", 0, 0).astype(jnp.float32)
    grad_small = jnp.transpose(swapped[:, 0], (0, 2, 1))
    grad_up = swapped[:, 1].reshape(4 * rows, slab).T
    grad_down = wide_block[:rows].T
    return (
        output,
        grad_tokens,
        totals[0],
        totals[1],
        grad_small[0],
        grad_small[1],
        grad_small[2],
        time_grads(all_times, notes[:, 4], rows),
        time_grads(all_times, notes[:, 5], rows),
        grad_small[3],
        grad_up,
        grad_down,
        totals[2, :entries].reshape(table),
        totals[3, :entries].reshape(table),
    )


def by_collectives(
    tokens, time_vec, grid, cotangent, gain_attn, gain_mlp, w_query, w_key, w_value, w_time_query, w_time_value, w_out,
    w_up, w_down, bias_rows, bias_cols,
):
    images, slots, width = tokens.shape
    cols = w_query.shape[1]
    mine_times, terms = time_terms(time_vec, w_time_query, w_time_value)
    terms = lax.psum(terms, "inner").reshape(-1, 2, cols)
    terms = lax.all_gather(terms, "dp", axis=2, tiled=True)
    here = (lax.axis_index("dp") * lax.psum(1, "inner") + lax.axis_index("inner")) * images
    terms = lax.dynamic_slice_in_dim(terms, here, images, axis=0)

    def whole(shard):
        part = lax.all_gather(shard, "inner", axis=0, tiled=True)
        return lax.all_gather(part, "dp", axis=1, tiled=True).T

    def shares(grad):
        part = lax.psum_scatter(grad.T, "inner", scatter_dimension=0, tiled=True)
        return lax.psum_scatter(part.astype(jnp.float32), "dp", scatter_dimension=1, tiled=True)

    turned = tuple(whole(shard) for shard in (w_query, w_key, w_value, w_out, w_down, w_up))
    output, grad_tokens, sums, grads = layer(
        tokens, grid, cotangent, gain_attn, gain_mlp, bias_rows, bias_cols, turned, terms[:, 0], terms[:, 1]
    )
    grad_query, grad_key, grad_value, grad_out, grad_down, grad_up = (shares(grad) for grad in grads)
    gain_a, gain_m, rows_table, cols_table = lax.psum(sums[:4], AXES)
    slot_queries, slot_values = (lax.all_gather(value, AXES, axis=0, tiled=True) for value in sums[4:])
    return (
        output, grad_tokens, gain_a, gain_m, grad_query, grad_key, grad_value,
        time_grads(mine_times, slot_queries, cols), time_grads(mine_times, slot_values, cols),
        grad_out, grad_up, grad_down, rows_table, cols_table,
    )


def solution(mesh):
    def local(*args):
        tokens, w_query = args[0], args[6]
        rings = dict(mesh.shape) == {"dp": SPOTS, "inner": 4} and tokens.shape[0] == 1
        rings = rings and w_query.shape[1] % 48 == 0 and tokens.shape[2] % 128 == 0
        return (by_rings if rings else by_collectives)(*args)

    data, weight = P(AXES, None, None), P("inner", "dp")
    return jax.shard_map(
        local,
        mesh=mesh,
        in_specs=(data, P(AXES, None), P(AXES, None), data, P(), P(), *(weight,) * 8, P(), P()),
        out_specs=(data, data, P(), P(), *(weight,) * 8, P(), P()),
        check_vma=False,
    )
```

```python
from functools import partial

import jax
import jax.numpy as jnp
from jax import lax
from jax.experimental import pallas as pl
from jax.experimental.pallas import tpu as pltpu
from jax.sharding import PartitionSpec as P

GS = 32
EPSILON = 1e-05
PRECISE = lax.Precision.HIGHEST
MESH = pl.DeviceIdType.MESH
AXES = ("dp", "inner")
SPOTS = 8


def place():
    dp, inner = lax.axis_index("dp"), lax.axis_index("inner")
    z, y = dp // 2, dp % 2
    return inner // 2, inner % 2, z + y * (7 - 2 * z)


def owner(x, core, spot):
    y = spot // 4
    z = spot + y * (7 - 2 * spot)
    return z * 2 + y, x * 2 + core


def ship(src, dst, send_sem, recv_sem, target):
    return pltpu.make_async_remote_copy(
        src_ref=src, dst_ref=dst, send_sem=send_sem, recv_sem=recv_sem, device_id=target, device_id_type=MESH
    )


def arrive(ref, sem):
    pltpu.make_async_copy(ref, ref, sem).wait()


def peers():
    x, core, spot = place()
    turn = 1 - 2 * core
    return (
        owner(x, core, (spot + turn + 8) % 8),
        owner(x, core, (spot - turn + 8) % 8),
        owner(1 - x, core, spot),
        owner(x, 1 - core, spot),
    )


def greet():
    barrier = pltpu.get_barrier_semaphore()
    for target in peers():
        pl.semaphore_signal(barrier, inc=1, device_id=target, device_id_type=MESH)
    pl.semaphore_wait(barrier, 4)


def every(count, body):
    def step(k, carry):
        body(k)
        return carry

    lax.fori_loop(0, count, step, 0)


class Gather:
    def __init__(self, own, home, pieces, early, ring_send, ring_recv, side_send, side_recv, pair_send, pair_recv):
        self.own, self.home, self.pieces, self.early = own, home, pieces, early
        self.ring, self.side, self.pair = (ring_send, ring_recv), (side_send, side_recv), (pair_send, pair_recv)
        self.x, self.core, self.spot = place()
        self.turn = 1 - 2 * self.core
        self.next, unused, self.across, self.partner = peers()
        self.order = [*range(early, pieces), *range(early)]

    @staticmethod
    def semaphores(pieces, early):
        dma = pltpu.SemaphoreType.DMA
        shapes = ((SPOTS - 1, pieces + early), (SPOTS, pieces), (SPOTS, 2 * pieces))
        return [dma(shape) for shape in shapes for twice in range(2)]

    def sent(self, pair, ref, slot, target, src=None):
        return ship(ref if src is None else src, ref, pair[0].at[slot], pair[1].at[slot], target)

    def who(self, step, plane):
        source = (self.spot - self.turn * step + 16) % 8
        return owner(self.x if plane == 0 else 1 - self.x, self.core, source)

    def start(self, own_sem):
        me = self.who(0, 0)
        for k in range(self.early):
            self.sent(self.side, self.home(k, me), (0, k), self.across, self.own(k)).start()
        for k in self.order:
            ref, src = self.home(k, me), self.own(k)
            self.sent(self.ring, ref, (0, k), self.next, src).start()
            if k >= self.early:
                self.sent(self.side, ref, (0, k), self.across, src).start()
        for k in self.order:
            ref, src = self.home(k, me), self.own(k)
            self.sent(self.pair, ref, (0, k), self.partner, src).start()
            pltpu.make_async_copy(src, ref, own_sem.at[k]).start()

    def kept(self, own_sem):
        for k in range(self.pieces):
            pltpu.make_async_copy(self.own(k), self.home(k, self.who(0, 0)), own_sem.at[k]).wait()

    def step(self, step):
        @pl.when(step > 0)
        def _():
            for k in self.order:
                ref = self.home(k, self.who(step, 0))
                arrive(ref, self.ring[1].at[step - 1, k])

                @pl.when(step < SPOTS - 1)
                def _():
                    self.sent(self.ring, ref, (step, k), self.next).start()

                if k >= self.early:
                    self.sent(self.side, ref, (step, k), self.across).start()
                self.sent(self.pair, ref, (step, k), self.partner).start()

        for k in range(self.early):
            ref = self.home(k, self.who(step, 1))

            @pl.when(step == 0)
            def _():
                arrive(ref, self.side[1].at[step, k])

            @pl.when(step > 0)
            def _():
                arrive(ref, self.ring[1].at[step - 1, self.pieces + k])

            @pl.when(step < SPOTS - 1)
            def _():
                self.sent(self.ring, ref, (step, self.pieces + k), self.next).start()

            self.sent(self.pair, ref, (step, self.pieces + k), self.partner).start()

        @pl.when(step > 0)
        def _():
            self.crossed(step - 1)

    def crossed(self, step):
        for k in range(self.early, self.pieces):
            ref = self.home(k, self.who(step, 1))
            arrive(ref, self.side[1].at[step, k])
            self.sent(self.pair, ref, (step, self.pieces + k), self.partner).start()

    def all_here(self):
        def last(step):
            source = (self.spot + self.turn * step + 16) % 8
            for plane in range(2):
                who = owner(self.x if plane == 0 else 1 - self.x, 1 - self.core, source)
                for k in range(self.pieces):
                    arrive(self.home(k, who), self.pair[1].at[step, plane * self.pieces + k])

        every(SPOTS, last)

    def drain(self):
        def last(step):
            for plane in range(2):
                for k in range(self.pieces):
                    mine = self.home(k, self.who(step, plane))
                    self.sent(self.pair, mine, (step, plane * self.pieces + k), self.partner).wait_send()
            for k in range(self.pieces):
                ref = self.home(k, self.who(step, 0))

                @pl.when(step < SPOTS - 1)
                def _():
                    self.sent(self.ring, ref, (step, k), self.next).wait_send()

                if k >= self.early:
                    self.sent(self.side, ref, (step, k), self.across).wait_send()
                else:

                    @pl.when(step == 0)
                    def _():
                        self.sent(self.side, ref, (step, k), self.across).wait_send()

            for k in range(self.early):
                ref = self.home(k, self.who(step, 1))

                @pl.when(step < SPOTS - 1)
                def _():
                    self.sent(self.ring, ref, (step, self.pieces + k), self.next).wait_send()

        every(SPOTS, last)


def nt(a, b):
    return lax.dot_general(a, b, (((1,), (1,)), ((), ())), preferred_element_type=jnp.float32)


def nn(a, b):
    return lax.dot_general(a, b, (((1,), (0,)), ((), ())), preferred_element_type=jnp.float32)


def tn(a, b):
    return lax.dot_general(a, b, (((0,), (0,)), ((), ())), preferred_element_type=jnp.float32)


def forward_kernel(
    small_early, early, scale, small_block, block, times, w_times, normed, squares, hots, mask, down_out, up_out,
    turned_out, times_out, queries, keys, values, probs, attended, shards, turned, time_buf, term_buf, terms, own_sem,
    turn_sem, time_send, time_recv, term_send, term_recv, *sems,
):
    x, core, spot = place()
    me = owner(x, core, spot)
    here = me[0] * 4 + me[1]
    rows, width = small_block.shape
    size, slab = rows // 2, width // 4
    barrier = pltpu.get_barrier_semaphore()

    def other(k):
        there = (here + k) % 32
        return there, (there // 4, there % 4)

    def signal(k):
        pl.semaphore_signal(barrier, inc=1, device_id=other(k + 1)[1], device_id_type=MESH)

    every(31, signal)
    pl.semaphore_wait(barrier, 31)

    def time_copy(k):
        there, target = other(k + 1)
        return ship(times.at[target[1]], time_buf.at[here], time_send.at[k], time_recv.at[k], target)

    def term_copy(k):
        there, target = other(k + 1)
        return ship(term_buf.at[there], terms.at[here], term_send.at[k], term_recv.at[k], target)

    def project():
        every(31, lambda k: arrive(time_buf.at[(here + 31 - k) % 32], time_recv.at[k]))
        known = time_buf[...].reshape(32, time_buf.shape[2])
        times_out[...] = known
        found = jnp.dot(known.astype(jnp.bfloat16), w_times[...], preferred_element_type=jnp.float32)
        term_buf[...] = found.reshape(32, 1, found.shape[1])
        every(31, lambda k: term_copy(k).start())
        terms[here] = term_buf[here]

    every(31, lambda k: time_copy(k).start())
    time_buf[here] = times[me[1]]

    small_bounds = ((0, small_early), (small_early, rows - small_early))
    bounds = ((0, early), (early, rows - early), (rows, rows))

    def small_home(k, who):
        lo, span = small_bounds[k]
        return shards.at[who[1], pl.ds(who[0] * rows + lo, span), :]

    def home(k, who):
        j, i = who
        if k == 0:
            return down_out.at[pl.ds(j * rows, early), pl.ds(i * width, width)]
        if k == 1:
            return down_out.at[pl.ds(j * rows + early, rows - early), pl.ds(i * width, width)]
        return up_out.at[pl.ds((j * 4 + i) * rows, rows), :]

    small = Gather(lambda k: small_block.at[pl.ds(*small_bounds[k]), :], small_home, 2, 1, *sems[:6])
    large = Gather(lambda k: block.at[pl.ds(*bounds[k]), :], home, 3, 1, *sems[6:])

    def keep(p, k):
        at = pl.ds(pl.multiple_of(p * rows, 16), rows)
        return pltpu.make_async_copy(turned.at[p % 2, k], turned_out.at[k, at, :], turn_sem.at[p % 2, k])

    def heads(p):
        at = pl.ds(pl.multiple_of(p * rows, 16), rows)

        @pl.when(p >= 2)
        def _():
            for k in range(4):
                keep(p - 2, k).wait()

        weights = []
        for k in range(4):
            part = slice(k * slab, (k + 1) * slab)
            weights.append(jnp.concatenate([shards[i, at, :][:, part] for i in range(4)], axis=1))
            turned[p % 2, k] = weights[k]
            keep(p, k).start()
        known = normed[...]
        hot = hots[...]
        term = terms[4 * p] + terms[4 * p + 1] + terms[4 * p + 2] + terms[4 * p + 3]
        query = (nt(known, weights[0]) + term[:, :rows]).astype(jnp.bfloat16)
        key = nt(known, weights[1]).astype(jnp.bfloat16)
        value = (nt(known, weights[2]) + term[:, rows : 2 * rows]).astype(jnp.bfloat16)
        queries[p] = query
        keys[p] = key
        values[p] = value
        outs = []
        for t in range(2):
            part = slice(t * size, (t + 1) * size)
            place_terms = sum(nn(hot, squares[k, 2 * p + t]) for k in range(3))
            high = place_terms.astype(jnp.bfloat16)
            rest = (place_terms - high.astype(jnp.float32)).astype(jnp.bfloat16)
            scores = nt(query[:, part], key[:, part]) * scale + (nt(high, hot) + nt(rest, hot))
            scores = jnp.where(mask[...] > 0.0, scores, -1000000000.0)
            expo = jnp.exp(scores - jnp.max(scores, axis=-1, keepdims=True))
            low = (expo / jnp.sum(expo, axis=-1, keepdims=True)).astype(jnp.bfloat16)
            probs[2 * p + t] = low
            outs.append(nn(low, value[:, part]))
        attended[p] = jnp.concatenate(outs, axis=1).astype(jnp.bfloat16)

    small.start(own_sem.at[0])

    def first(step):
        small.step(step)

        @pl.when(step == 3)
        def _():
            project()

    every(SPOTS, first)
    large.start(own_sem.at[1])
    small.crossed(SPOTS - 1)
    large.step(0)
    small.all_here()
    small.kept(own_sem.at[0])
    every(31, lambda k: arrive(terms.at[(here + 31 - k) % 32], term_recv.at[k]))
    large.step(1)

    def second(n):
        step = n + 2
        large.step(step)

        @pl.when(step < 4)
        def _():
            heads(2 * n)

        heads(jnp.where(step < 4, 2 * n + 1, step))

    every(SPOTS - 2, second)
    large.crossed(SPOTS - 1)
    for p in (SPOTS - 2, SPOTS - 1):
        for k in range(4):
            keep(p, k).wait()
    large.all_here()
    large.kept(own_sem.at[1])

    def sent(k):
        time_copy(k).wait_send()
        term_copy(k).wait_send()

    every(31, sent)
    small.drain()
    large.drain()


def gathered_forward(small_block, block, times, w_times, normed, squares, hots, mask, scale):
    rows, width = small_block.shape
    slots, lanes = normed.shape[0], times.shape[2]
    dma = pltpu.SemaphoreType.DMA
    vmem, far = pl.BlockSpec(memory_space=pltpu.VMEM), pl.BlockSpec(memory_space=pl.ANY)
    low = block.dtype
    pair = jax.ShapeDtypeStruct((SPOTS, slots, rows), low)
    terms = (32, 1, w_times.shape[1])
    return pl.pallas_call(
        partial(forward_kernel, rows * 4 // 9, rows * 8 // 9, scale),
        out_shape=(
            jax.ShapeDtypeStruct((SPOTS * rows, 4 * width), low),
            jax.ShapeDtypeStruct((32 * rows, width), low),
            jax.ShapeDtypeStruct((4, SPOTS * rows, width), low),
            jax.ShapeDtypeStruct((32, lanes), jnp.float32),
            pair,
            pair,
            pair,
            jax.ShapeDtypeStruct((2 * SPOTS, slots, slots), low),
            pair,
        ),
        in_specs=[vmem] * 8,
        out_specs=(far,) * 3 + (vmem,) * 6,
        scratch_shapes=[
            pltpu.VMEM((4, SPOTS * rows, width), low),
            pltpu.VMEM((2, 4, rows, width), low),
            pltpu.VMEM((32, 1, lanes), jnp.float32),
            pltpu.VMEM(terms, jnp.float32),
            pltpu.VMEM(terms, jnp.float32),
            dma((2, 3)),
            dma((2, 4)),
            dma((31,)),
            dma((31,)),
            dma((31,)),
            dma((31,)),
            *Gather.semaphores(2, 1),
            *Gather.semaphores(3, 1),
        ],
        compiler_params=pltpu.CompilerParams(collective_id=0, has_side_effects=True, vmem_limit_bytes=60 << 20),
        name="attention_forward",
    )(small_block, block, times, w_times, normed, squares, hots, mask)


def pile(target, sources, size):
    tile = 16

    def body(k):
        total = None
        for ref, base in sources:
            piece = ref[pl.ds(pl.multiple_of(base + k * tile, 16), tile), :].astype(jnp.float32)
            total = piece if total is None else total + piece
        ref, base = target
        ref[pl.ds(pl.multiple_of(base + k * tile, 16), tile), :] = total.astype(ref.dtype)

    every(size // tile, body)


class Scatter:
    def __init__(
        self, home, parts, rows, early, result, pair_buf, ring_buf, side_buf, last_buf, own_buf, own_sem, ring_send,
        ring_recv, side_send, side_recv, last_send, last_recv, pair_send, pair_recv,
    ):
        self.home, self.parts, self.rows, self.early = home, parts, rows, early
        self.block = parts * rows
        self.result = result
        self.pair_buf, self.ring_buf, self.side_buf, self.last_buf, self.own_buf = (
            pair_buf, ring_buf, side_buf, last_buf, own_buf,
        )
        self.own_sem = own_sem
        self.ring, self.side, self.pair = (ring_send, ring_recv), (side_send, side_recv), (pair_send, pair_recv)
        self.last = (last_send, last_recv)
        self.x, self.core, self.spot = place()
        self.turn = 1 - 2 * self.core
        self.next, unused, self.across, self.partner = peers()

    @staticmethod
    def scratch(parts, rows, early, width, low):
        dma = pltpu.SemaphoreType.DMA
        block = parts * rows
        return [
            pltpu.VMEM((SPOTS, 2, block, width), low),
            pltpu.VMEM((SPOTS - 1, block + early, width), low),
            pltpu.VMEM((SPOTS, block - early, width), low),
            pltpu.VMEM((early, width), low),
            pltpu.VMEM((2, 2, block, width), low),
            dma((2, 2, parts)),
            dma((SPOTS - 1, 3)),
            dma((SPOTS - 1, 3)),
            dma((SPOTS,)),
            dma((SPOTS,)),
            dma((1,)),
            dma((1,)),
            dma((SPOTS, 2, parts)),
            dma((SPOTS, 2, parts)),
        ]

    def span(self, part):
        return pl.ds(part * self.rows, self.rows)

    def pair_copy(self, step, plane, part):
        goal = (self.spot + self.turn * (1 + step) + 16) % 8
        who = owner(self.x if plane == 0 else 1 - self.x, 1 - self.core, goal)
        return ship(
            self.home(part, who),
            self.pair_buf.at[step, plane, self.span(part), :],
            self.pair[0].at[step, plane, part],
            self.pair[1].at[step, plane, part],
            self.partner,
        )

    def begin(self):
        def give(step):
            for plane in (1, 0):
                for part in range(self.parts):
                    self.pair_copy(step, plane, part).start()

        every(SPOTS, give)
        self.fetch(0)

    def loads(self, step, plane):
        goal = (self.spot - self.turn * (1 + step) + 16) % 8
        who = owner(self.x if plane == 0 else 1 - self.x, self.core, goal)
        return [
            pltpu.make_async_copy(
                self.home(part, who),
                self.own_buf.at[step % 2, plane, self.span(part), :],
                self.own_sem.at[step % 2, plane, part],
            )
            for part in range(self.parts)
        ]

    def fetch(self, step):
        for plane in (1, 0):
            for copy in self.loads(step, plane):
                copy.start()

    def ready(self, step, plane):
        for copy in self.loads(step, plane):
            copy.wait()
        for part in range(self.parts):
            arrive(self.pair_buf.at[step, plane, self.span(part), :], self.pair[1].at[step, plane, part])

    def side_copy(self, step):
        src = self.pair_buf.at[step, 1, pl.ds(self.early, self.block - self.early), :]
        return ship(src, self.side_buf.at[step], self.side[0].at[step], self.side[1].at[step], self.across)

    def lane(self, n):
        return (
            (0, 0, 0, self.early),
            (0, self.early, self.early, self.block - self.early),
            (1, 0, self.block, self.early),
        )[n]

    def ring_copy(self, step, n):
        plane, lo, base, size = self.lane(n)
        return ship(
            self.pair_buf.at[step, plane, pl.ds(lo, size), :],
            self.ring_buf.at[step, pl.ds(base, size), :],
            self.ring[0].at[step, n],
            self.ring[1].at[step, n],
            self.next,
        )

    def sources(self, step, n, ring):
        plane, lo, base, size = self.lane(n)
        refs = [(self.own_buf.at[step % 2, plane], lo), (self.pair_buf.at[step, plane], lo)]
        if n == 1:
            refs.append((self.side_buf.at[step], 0))
        if ring:
            refs.append((self.ring_buf.at[step - 1], base))
        return refs

    def across_part(self, step):
        self.ready(step, 1)
        held = self.pair_buf.at[step, 1]
        mine = self.own_buf.at[step % 2, 1]
        pile((held, self.early), [(mine, self.early), (held, self.early)], self.block - self.early)
        self.side_copy(step).start()
        self.ready(step, 0)

    def step(self, step):
        self.across_part(step)
        self.fetch(step + 1)
        for n in range(3):
            plane, lo, base, size = self.lane(n)
            if n == 1:
                arrive(self.side_buf.at[step], self.side[1].at[step])

            @pl.when(step == 0)
            def _():
                pile((self.pair_buf.at[step, plane], lo), self.sources(step, n, False), size)

            @pl.when(step > 0)
            def _():
                arrive(self.ring_buf.at[step - 1, pl.ds(base, size), :], self.ring[1].at[step - 1, n])
                pile((self.pair_buf.at[step, plane], lo), self.sources(step, n, True), size)

            self.ring_copy(step, n).start()

    def finish(self):
        step = SPOTS - 1
        self.across_part(step)
        for n in (2, 1, 0):
            plane, lo, base, size = self.lane(n)
            arrive(self.ring_buf.at[step - 1, pl.ds(base, size), :], self.ring[1].at[step - 1, n])
            refs = self.sources(step, n, True)
            if n == 2:
                pile((self.pair_buf.at[step, 1], 0), refs, size)
                src = self.pair_buf.at[step, 1, pl.ds(0, size), :]
                over = ship(src, self.last_buf, self.last[0].at[0], self.last[1].at[0], self.across)
                over.start()
                continue
            if n == 1:
                arrive(self.side_buf.at[step], self.side[1].at[step])
            else:
                arrive(self.last_buf, self.last[1].at[0])
                refs.append((self.last_buf, 0))
            pile((self.result, lo), refs, size)
        over.wait_send()

        def sent(step):
            for plane in range(2):
                for part in range(self.parts):
                    self.pair_copy(step, plane, part).wait_send()
            self.side_copy(step).wait_send()

            @pl.when(step < SPOTS - 1)
            def _():
                for n in range(3):
                    self.ring_copy(step, n).wait_send()

        every(SPOTS, sent)


def backward_kernel(
    early, scale, down_in, up_in, small_in, normed, attended, grad_mixed, grad_attended, queries, keys, values, probs, hots,
    result, small_out,
    grad_normed, squares, sums, weights, load_sem, grads, grad_sem, *scratch,
):
    rows, width = result.shape[0] // 2, result.shape[1]
    size = rows // 2
    slab = width // 4
    greet()
    loads = [pltpu.make_async_copy(small_in.at[k], weights.at[k], load_sem.at[k]) for k in range(3)]
    for copy in loads:
        copy.start()

    def home(part, who):
        j, i = who
        if part == 0:
            return down_in.at[pl.ds(j * rows, rows), pl.ds(i * width, width)]
        return up_in.at[pl.ds((j * 4 + i) * rows, rows), :]

    scatter = Scatter(home, 2, rows, early, result, *scratch)
    scatter.begin()
    grad_normed[...] = jnp.zeros_like(grad_normed)

    def keep(p, k):
        return pltpu.make_async_copy(
            grads.at[p % 2, k], small_out.at[k, pl.ds(pl.multiple_of(p * rows, 16), rows), :], grad_sem.at[p % 2, k]
        )

    def heads(p):
        query, key, value, above = queries[p], keys[p], values[p], grad_attended[p]
        hot = hots[...]
        parts = ([], [], [])
        for t in range(2):
            part = slice(t * size, (t + 1) * size)
            low = probs[2 * p + t]
            wide = low.astype(jnp.float32)
            grad_probs = nt(above[:, part], value[:, part])
            inner = jnp.sum(wide * grad_probs, axis=-1, keepdims=True)
            grad_scores = (wide * (grad_probs - inner)).astype(jnp.bfloat16)
            parts[0].append(nn(grad_scores, key[:, part]) * scale)
            parts[1].append(tn(grad_scores, query[:, part]) * scale)
            parts[2].append(tn(low, above[:, part]))
            across = nn(grad_scores, hot)
            high = across.astype(jnp.bfloat16)
            rest = (across - high.astype(jnp.float32)).astype(jnp.bfloat16)
            squares[2 * p + t] = tn(hot, high) + tn(hot, rest)

        @pl.when(p >= 2)
        def _():
            for k in range(4):
                keep(p - 2, k).wait()

        known = normed[...]
        at = pl.ds(pl.multiple_of(p * rows, 16), rows)
        total = None
        turned = []
        for k in range(3):
            grad = jnp.concatenate(parts[k], axis=1).astype(jnp.bfloat16)
            sums[k, p] = jnp.sum(grad.astype(jnp.float32), axis=0, keepdims=True)
            turned.append(tn(grad, known).astype(jnp.bfloat16))
            term = nn(grad, weights[k, at, :])
            total = term if total is None else total + term
        grad_normed[...] += total
        turned.append(tn(grad_mixed[p], attended[...]).astype(jnp.bfloat16))
        for k in range(4):
            part = slice(k * slab, (k + 1) * slab)
            grads[p % 2, k] = jnp.concatenate([rows_of[:, part] for rows_of in turned], axis=1)
            keep(p, k).start()

    def work(step):
        @pl.when(step < SPOTS - 1)
        def _():
            scatter.step(step)

        @pl.when(step == 0)
        def _():
            for copy in loads:
                copy.wait()

        heads(step)

    every(SPOTS, work)
    for p in (SPOTS - 2, SPOTS - 1):
        for k in range(4):
            keep(p, k).wait()
    scatter.finish()


def attention_backward(
    down, up, small, normed, attended, grad_mixed, grad_attended, queries, keys, values, probs, hots, scale
):
    rows, width = up.shape[0] // 32, up.shape[1]
    early = rows * 8 // 9
    slots = normed.shape[0]
    sides = hots.shape[1]
    low = up.dtype
    dma = pltpu.SemaphoreType.DMA
    vmem, far = pl.BlockSpec(memory_space=pltpu.VMEM), pl.BlockSpec(memory_space=pl.ANY)
    return pl.pallas_call(
        partial(backward_kernel, early, scale),
        out_shape=(
            jax.ShapeDtypeStruct((2 * rows, width), jnp.float32),
            jax.ShapeDtypeStruct((4, SPOTS * rows, width), low),
            jax.ShapeDtypeStruct((slots, width), jnp.float32),
            jax.ShapeDtypeStruct((2 * SPOTS, sides, sides), jnp.float32),
            jax.ShapeDtypeStruct((3, SPOTS, 1, rows), jnp.float32),
        ),
        in_specs=[far] * 3 + [vmem] * 9,
        out_specs=(vmem, far, vmem, vmem, vmem),
        scratch_shapes=[
            pltpu.VMEM((3, SPOTS * rows, width), low),
            dma((3,)),
            pltpu.VMEM((2, 4, rows, width), low),
            dma((2, 4)),
            *Scatter.scratch(2, rows, early, width, low),
        ],
        compiler_params=pltpu.CompilerParams(collective_id=2, has_side_effects=True, vmem_limit_bytes=63 << 20),
        name="attention_backward",
    )(down, up, small, normed, attended, grad_mixed, grad_attended, queries, keys, values, probs, hots)


def last_sums_kernel(early, small_in, out_in, extra_in, result, extra_out, own_sem, note_sems, scratch):
    x, core, spot = place()
    rows = result.shape[0]
    greet()

    def home(part, who):
        return small_in.at[who[1], pl.ds(who[0] * rows, rows), :]

    def note(k, who):
        return extra_out.at[who[0] * 4 + who[1]]

    scatter = Scatter(home, 1, rows, early, result, *scratch)
    scatter.begin()
    notes = Gather(lambda k: extra_in, note, 1, 1, *note_sems)
    notes.start(own_sem)

    def work(step):
        notes.step(step)

        @pl.when(step < SPOTS - 1)
        def _():
            scatter.step(step)

    every(SPOTS, work)
    scatter.finish()
    notes.all_here()
    notes.kept(own_sem)
    notes.drain()


def last_sums(small, extra):
    rows, width = small.shape[1] // SPOTS, small.shape[2]
    early = rows * 4 // 9
    low = small.dtype
    vmem, far = pl.BlockSpec(memory_space=pltpu.VMEM), pl.BlockSpec(memory_space=pl.ANY)

    def kernel(small_in, extra_in, result, extra_out, own_sem, *rest):
        last_sums_kernel(early, small_in, None, extra_in, result, extra_out, own_sem, rest[:6], rest[6:])

    return pl.pallas_call(
        kernel,
        out_shape=(
            jax.ShapeDtypeStruct((rows, width), jnp.float32),
            jax.ShapeDtypeStruct((32, *extra.shape), extra.dtype),
        ),
        in_specs=[far, vmem],
        out_specs=(vmem, vmem),
        scratch_shapes=[
            pltpu.SemaphoreType.DMA((1,)),
            *Gather.semaphores(1, 1),
            *Scatter.scratch(1, rows, early, width, low),
        ],
        compiler_params=pltpu.CompilerParams(collective_id=3, has_side_effects=True),
        name="last_sums",
    )(small, extra)


def layer_norm(matrix, gains):
    center = matrix - jnp.mean(matrix, axis=-1, keepdims=True)
    spread = jnp.mean(center * center, axis=-1, keepdims=True)
    return center * lax.rsqrt(spread + EPSILON) * gains


def slot_positions(grid, slots):
    heights = grid[:, 0]
    widths = grid[:, 1]
    length = heights * widths
    places = jnp.arange(slots, dtype=jnp.int32)
    usable = places[None, :] < length[:, None]
    clipped = jnp.minimum(places[None, :], length[:, None] - 1)
    return (usable, clipped // widths[:, None], clipped % widths[:, None])


def offset_table():
    shape = (GS, GS, 2 * GS - 1)
    source = lax.broadcasted_iota(jnp.int32, shape, 0)
    target = lax.broadcasted_iota(jnp.int32, shape, 1)
    offset = lax.broadcasted_iota(jnp.int32, shape, 2)
    return (source - target + (GS - 1) == offset).astype(jnp.float32)


def side_hot(places):
    sides = lax.broadcasted_iota(jnp.int32, (1, 1, GS), 2)
    return (places[:, :, None] == sides).astype(jnp.float32)


def position_bias(row_hot, col_hot, bias_rows, bias_cols, offset_hot):
    terms = []
    for hot_side, table in ((row_hot, bias_rows), (col_hot, bias_cols)):
        square = jnp.einsum("hd,rsd->hrs", table, offset_hot, precision=PRECISE)
        partial_rows = jnp.einsum("nir,hrs->nhis", hot_side, square, precision=PRECISE)
        terms.append(jnp.einsum("nhis,njs->nhij", partial_rows, hot_side, precision=PRECISE))
    return terms[0] + terms[1]


def bias_grads(grad_scores, row_hot, col_hot, offset_hot):
    results = []
    for hot_side in (row_hot, col_hot):
        partial_cols = jnp.einsum("nhij,njs->nhis", grad_scores, hot_side, precision=PRECISE)
        square = jnp.einsum("nir,nhis->hrs", hot_side, partial_cols, precision=PRECISE)
        results.append(jnp.einsum("hrs,rsd->hd", square, offset_hot, precision=PRECISE))
    return (results[0], results[1])


def masked_scores(queries, key_heads, position, usable):
    head_size = queries.shape[3]
    raw = jnp.einsum("nihe,njhe->nhij", queries, key_heads, preferred_element_type=jnp.float32)
    scores = raw * head_size ** (-0.5) + position
    return jnp.where(usable[:, None, None, :], scores, -1000000000.0)


def layer(tokens, grid, cotangent, gain_attn, gain_mlp, bias_rows, bias_cols, turned, time_query, time_value):
    images, slots, width = tokens.shape
    heads = bias_rows.shape[0]
    head_size = width // heads
    scale = head_size ** (-0.5)
    flat = images * slots
    gelu_tanh = partial(jax.nn.gelu, approximate=True)
    t_query, t_key, t_value, t_out, t_down, t_up = turned
    ahead = partial(jnp.einsum, "rd,ed->re", preferred_element_type=jnp.float32)
    back = partial(jnp.einsum, "re,ed->rd", preferred_element_type=jnp.float32)

    def outer(grads, values):
        return jnp.einsum("re,rd->ed", grads, values, preferred_element_type=jnp.float32).astype(jnp.bfloat16)

    inputs = tokens.astype(jnp.float32).reshape(flat, width)
    normed_attn = layer_norm(inputs, gain_attn).astype(jnp.bfloat16)
    shape = (images, slots, heads, head_size)
    queries = ahead(normed_attn, t_query).reshape(images, slots, width)
    queries = (queries + time_query[:, None, :]).astype(jnp.bfloat16).reshape(shape)
    key_heads = ahead(normed_attn, t_key).astype(jnp.bfloat16).reshape(shape)
    value_heads = ahead(normed_attn, t_value).reshape(images, slots, width)
    value_heads = (value_heads + time_value[:, None, :]).astype(jnp.bfloat16).reshape(shape)
    usable, row_place, col_place = slot_positions(grid, slots)
    offset_hot = offset_table()
    row_hot = side_hot(row_place)
    col_hot = side_hot(col_place)
    position = position_bias(row_hot, col_hot, bias_rows, bias_cols, offset_hot)
    scores = masked_scores(queries, key_heads, position, usable)
    maxima = jnp.max(scores, axis=-1, keepdims=True)
    expo = jnp.exp(scores - maxima)
    totals = jnp.sum(expo, axis=-1, keepdims=True)
    probs_low = (expo / totals).astype(jnp.bfloat16)
    attended = jnp.einsum("nhij,njhe->nihe", probs_low, value_heads, preferred_element_type=jnp.float32)
    attended = attended.astype(jnp.bfloat16).reshape(flat, width)
    mixed = inputs + ahead(attended, t_out)
    normed_mlp = layer_norm(mixed, gain_mlp).astype(jnp.bfloat16)
    up_proj = ahead(normed_mlp, t_up)
    hidden = gelu_tanh(up_proj).astype(jnp.bfloat16)
    keep_rows = usable.reshape(flat, 1)
    result = jnp.where(keep_rows, mixed + ahead(hidden, t_down), 0.0)
    output = result.astype(jnp.bfloat16).reshape(images, slots, width)
    upstream = jnp.where(keep_rows, cotangent.astype(jnp.float32).reshape(flat, width), 0.0)
    upstream_low = upstream.astype(jnp.bfloat16)
    grad_down = outer(upstream_low, hidden)
    grad_hidden = back(upstream_low, t_down)
    unused_gelu, gelu_back = jax.vjp(gelu_tanh, up_proj)
    grad_up_proj = gelu_back(grad_hidden)[0].astype(jnp.bfloat16)
    grad_up = outer(grad_up_proj, normed_mlp)
    grad_normed_mlp = back(grad_up_proj, t_up)
    unused_mlp, norm_mlp_back = jax.vjp(layer_norm, mixed, gain_mlp)
    grad_mixed_norm, grad_gain_mlp = norm_mlp_back(grad_normed_mlp)
    grad_mixed = upstream + grad_mixed_norm
    grad_mixed_low = grad_mixed.astype(jnp.bfloat16)
    grad_out = outer(grad_mixed_low, attended)
    grad_attended = back(grad_mixed_low, t_out).astype(jnp.bfloat16).reshape(shape)
    scores = masked_scores(queries, key_heads, position, usable)
    probs = jnp.exp(scores - maxima) / totals
    probs_low = probs.astype(jnp.bfloat16)
    grad_probs = jnp.einsum("nihe,njhe->nhij", grad_attended, value_heads, preferred_element_type=jnp.float32)
    inner_sum = jnp.sum(probs * grad_probs, axis=-1, keepdims=True)
    grad_scores = (probs * (grad_probs - inner_sum)).astype(jnp.bfloat16)
    grad_queries = jnp.einsum("nhij,njhe->nihe", grad_scores, key_heads, preferred_element_type=jnp.float32) * scale
    grad_queries = grad_queries.astype(jnp.bfloat16).reshape(images, slots, width)
    grad_keys = jnp.einsum("nhij,nihe->njhe", grad_scores, queries, preferred_element_type=jnp.float32) * scale
    grad_keys = grad_keys.astype(jnp.bfloat16).reshape(flat, width)
    grad_values = jnp.einsum("nhij,nihe->njhe", probs_low, grad_attended, preferred_element_type=jnp.float32)
    grad_values = grad_values.astype(jnp.bfloat16).reshape(images, slots, width)
    grad_rows_table, grad_cols_table = bias_grads(grad_scores.astype(jnp.float32), row_hot, col_hot, offset_hot)
    flat_queries = grad_queries.reshape(flat, width)
    flat_values = grad_values.reshape(flat, width)
    grad_query = outer(flat_queries, normed_attn)
    grad_key = outer(grad_keys, normed_attn)
    grad_value = outer(flat_values, normed_attn)
    slot_queries = jnp.sum(grad_queries.astype(jnp.float32), axis=1)
    slot_values = jnp.sum(grad_values.astype(jnp.float32), axis=1)
    grad_normed_attn = back(flat_queries, t_query) + back(grad_keys, t_key) + back(flat_values, t_value)
    unused_attn, norm_attn_back = jax.vjp(layer_norm, inputs, gain_attn)
    grad_inputs_norm, grad_gain_attn = norm_attn_back(grad_normed_attn)
    grad_tokens = (grad_mixed + grad_inputs_norm).astype(jnp.bfloat16).reshape(images, slots, width)
    return (
        output,
        grad_tokens,
        (grad_gain_attn, grad_gain_mlp, grad_rows_table, grad_cols_table, slot_queries, slot_values),
        (grad_query, grad_key, grad_value, grad_out, grad_down, grad_up),
    )


def time_terms(time_vec, w_time_query, w_time_value):
    all_times = lax.all_gather(time_vec, AXES, axis=0, tiled=True)
    rows = w_time_query.shape[0]
    mine = lax.dynamic_slice_in_dim(all_times, lax.axis_index("inner") * rows, rows, axis=1)
    both = jnp.concatenate([w_time_query, w_time_value], axis=1)
    return mine, jnp.dot(mine, both, preferred_element_type=jnp.float32)


def time_grads(mine, slot_sums, cols):
    column = lax.axis_index("dp") * cols
    picked = lax.dynamic_slice_in_dim(slot_sums, column, cols, axis=1)
    return jnp.einsum("nd,ne->de", mine.astype(jnp.float32), picked, precision=PRECISE)


def by_rings(
    tokens, time_vec, grid, cotangent, gain_attn, gain_mlp, w_query, w_key, w_value, w_time_query, w_time_value, w_out,
    w_up, w_down, bias_rows, bias_cols,
):
    images, slots, width = tokens.shape
    slab, rows = w_query.shape
    heads = bias_rows.shape[0]
    scale = (width // heads) ** (-0.5)
    gelu_tanh = partial(jax.nn.gelu, approximate=True)
    ahead = partial(jnp.einsum, "rd,ed->re", preferred_element_type=jnp.float32)
    back = partial(jnp.einsum, "re,ed->rd", preferred_element_type=jnp.float32)

    def outer(grads, values):
        return jnp.einsum("re,rd->ed", grads, values, preferred_element_type=jnp.float32).astype(jnp.bfloat16)

    small = jnp.concatenate([w_query.T, w_key.T, w_value.T, w_out.T], axis=1)
    swapped = lax.all_to_all(w_up.T.reshape(4, rows, slab), "inner", 0, 0)
    wide = jnp.transpose(swapped, (1, 0, 2)).reshape(rows, width)
    w_times = jnp.concatenate([w_time_query, w_time_value], axis=1)
    w_times = jnp.pad(w_times, ((0, -slab % 128), (0, -2 * rows % 128)))
    times = time_vec.astype(jnp.float32).reshape(4, 1, slab)
    times = jnp.pad(times, ((0, 0), (0, 0), (0, -slab % 128)))
    inputs = tokens.astype(jnp.float32).reshape(slots, width)
    normed_attn = layer_norm(inputs, gain_attn).astype(jnp.bfloat16)
    usable, row_place, col_place = slot_positions(grid, slots)
    offset_hot = offset_table()
    hot = jnp.concatenate([side_hot(row_place)[0], side_hot(col_place)[0]], axis=1)
    square = [
        jnp.einsum("hd,rsd->hrs", table, offset_hot, precision=PRECISE) for table in (bias_rows, bias_cols)
    ]
    square = jnp.concatenate(
        [jnp.pad(square[0], ((0, 0), (0, 0), (0, GS))), jnp.pad(square[1], ((0, 0), (0, 0), (GS, 0)))], axis=1
    )
    first = lax.reduce_precision(square, 8, 7)
    second = lax.reduce_precision(square - first, 8, 7)
    squares = jnp.stack([first, second, square - first - second]).astype(jnp.bfloat16)
    hot = hot.astype(jnp.bfloat16)
    mask = usable.astype(jnp.float32)
    block = jnp.concatenate([w_down.T, wide], axis=0)
    t_down, t_up, t_small, all_times, queries, keys, values, probs, attended = gathered_forward(
        small, block, times, w_times, normed_attn, squares, hot, mask, scale
    )
    all_times = all_times[:, :slab]
    attended = jnp.transpose(attended, (1, 0, 2)).reshape(slots, width)
    mixed = inputs + ahead(attended, t_small[3])
    normed_mlp = layer_norm(mixed, gain_mlp).astype(jnp.bfloat16)
    up_proj = ahead(normed_mlp, t_up)
    hidden = gelu_tanh(up_proj).astype(jnp.bfloat16)
    keep_rows = usable.reshape(slots, 1)
    result = jnp.where(keep_rows, mixed + ahead(hidden, t_down), 0.0)
    output = result.astype(jnp.bfloat16).reshape(images, slots, width)
    upstream = jnp.where(keep_rows, cotangent.astype(jnp.float32).reshape(slots, width), 0.0)
    upstream_low = upstream.astype(jnp.bfloat16)
    grad_down = outer(upstream_low, hidden)
    grad_hidden = back(upstream_low, t_down)
    unused_gelu, gelu_back = jax.vjp(gelu_tanh, up_proj)
    grad_up_proj = gelu_back(grad_hidden)[0].astype(jnp.bfloat16)
    grad_up = outer(grad_up_proj, normed_mlp)
    grad_normed_mlp = back(grad_up_proj, t_up)
    unused_mlp, norm_mlp_back = jax.vjp(layer_norm, mixed, gain_mlp)
    grad_mixed_norm, grad_gain_mlp = norm_mlp_back(grad_normed_mlp)
    grad_mixed = upstream + grad_mixed_norm
    grad_mixed_low = grad_mixed.astype(jnp.bfloat16)
    grad_attended = back(grad_mixed_low, t_small[3]).astype(jnp.bfloat16)
    grad_attended = jnp.transpose(grad_attended.reshape(slots, SPOTS, rows), (1, 0, 2))
    mixed_pairs = jnp.transpose(grad_mixed_low.reshape(slots, SPOTS, rows), (1, 0, 2))
    wide_block, small_grads, grad_normed_attn, table_squares, slot_sums = attention_backward(
        grad_down, grad_up, t_small, normed_attn, attended, mixed_pairs, grad_attended, queries, keys, values, probs, hot,
        scale,
    )
    parted = jnp.transpose(wide_block[rows:].astype(jnp.bfloat16).reshape(rows, 4, slab), (1, 0, 2))
    swapped = lax.all_to_all(parted, "inner", 0, 0).astype(jnp.float32)
    unused_attn, norm_attn_back = jax.vjp(layer_norm, inputs, gain_attn)
    grad_inputs_norm, grad_gain_attn = norm_attn_back(grad_normed_attn)
    grad_tokens = (grad_mixed + grad_inputs_norm).astype(jnp.bfloat16).reshape(images, slots, width)
    tables = [
        jnp.einsum("hrs,rsd->hd", table_squares[:, cut, cut], offset_hot, precision=PRECISE)
        for cut in (slice(0, GS), slice(GS, 2 * GS))
    ]
    own = (grad_gain_attn, grad_gain_mlp, *tables, slot_sums[0], slot_sums[2])
    notes = jnp.stack([jnp.pad(value.reshape(-1), (0, width - value.size)) for value in own])
    notes = jnp.pad(notes, ((0, 2), (0, 0)))
    small_block, notes = last_sums(small_grads, notes)
    totals = notes[:, :4].sum(axis=0)
    entries = bias_rows.size
    table = bias_rows.shape
    grad_small = [small_block[:, slab * k : slab * (k + 1)].T for k in range(4)]
    grad_up = swapped.reshape(4 * rows, slab).T
    grad_down = wide_block[:rows].T
    return (
        output,
        grad_tokens,
        totals[0],
        totals[1],
        grad_small[0],
        grad_small[1],
        grad_small[2],
        time_grads(all_times, notes[:, 4], rows),
        time_grads(all_times, notes[:, 5], rows),
        grad_small[3],
        grad_up,
        grad_down,
        totals[2, :entries].reshape(table),
        totals[3, :entries].reshape(table),
    )


def by_collectives(
    tokens, time_vec, grid, cotangent, gain_attn, gain_mlp, w_query, w_key, w_value, w_time_query, w_time_value, w_out,
    w_up, w_down, bias_rows, bias_cols,
):
    images, slots, width = tokens.shape
    cols = w_query.shape[1]
    mine_times, terms = time_terms(time_vec, w_time_query, w_time_value)
    terms = lax.psum(terms, "inner").reshape(-1, 2, cols)
    terms = lax.all_gather(terms, "dp", axis=2, tiled=True)
    here = (lax.axis_index("dp") * lax.psum(1, "inner") + lax.axis_index("inner")) * images
    terms = lax.dynamic_slice_in_dim(terms, here, images, axis=0)

    def whole(shard):
        part = lax.all_gather(shard, "inner", axis=0, tiled=True)
        return lax.all_gather(part, "dp", axis=1, tiled=True).T

    def shares(grad):
        part = lax.psum_scatter(grad.T, "inner", scatter_dimension=0, tiled=True)
        return lax.psum_scatter(part.astype(jnp.float32), "dp", scatter_dimension=1, tiled=True)

    turned = tuple(whole(shard) for shard in (w_query, w_key, w_value, w_out, w_down, w_up))
    output, grad_tokens, sums, grads = layer(
        tokens, grid, cotangent, gain_attn, gain_mlp, bias_rows, bias_cols, turned, terms[:, 0], terms[:, 1]
    )
    grad_query, grad_key, grad_value, grad_out, grad_down, grad_up = (shares(grad) for grad in grads)
    gain_a, gain_m, rows_table, cols_table = lax.psum(sums[:4], AXES)
    slot_queries, slot_values = (lax.all_gather(value, AXES, axis=0, tiled=True) for value in sums[4:])
    return (
        output, grad_tokens, gain_a, gain_m, grad_query, grad_key, grad_value,
        time_grads(mine_times, slot_queries, cols), time_grads(mine_times, slot_values, cols),
        grad_out, grad_up, grad_down, rows_table, cols_table,
    )


def solution(mesh):
    def local(*args):
        tokens, w_query = args[0], args[6]
        rings = dict(mesh.shape) == {"dp": SPOTS, "inner": 4} and tokens.shape[0] == 1
        rings = rings and w_query.shape[1] % 48 == 0 and tokens.shape[2] % 128 == 0
        return (by_rings if rings else by_collectives)(*args)

    data, weight = P(AXES, None, None), P("inner", "dp")
    return jax.shard_map(
        local,
        mesh=mesh,
        in_specs=(data, P(AXES, None), P(AXES, None), data, P(), P(), *(weight,) * 8, P(), P()),
        out_specs=(data, data, P(), P(), *(weight,) * 8, P(), P()),
        check_vma=False,
    )
```
